128 devices in a mesh: seq: 16 (over x_lo, z, core), head: 4 (over y), batch: 2 (over x_hi).
Axes of the slice: x: 4 (x_hi: 2, x_lo: 2; x = x_hi * 2 + x_lo), y: 4, z: 4, core: 2. Of those that a mesh axis runs over, the one named last changes fastest.
Arguments:
- tokens: bfloat16 [32768, 2048], P(('batch', 'seq')), parts along dimension 0, may hold values from -6 to 6
- neighbor_bank: bfloat16 [512, 256, 2048], P(('batch', 'seq')), parts along dimension 0, may hold values from -2100 to 2100
- slots: int32 [512], P(('batch', 'seq')), parts along dimension 0, may hold values from 0 to 15
- w_query: bfloat16 [2048, 2048], P('seq', 'head'), may hold values from -0.125 to 0.125
- w_key: bfloat16 [2048, 2048], P('seq', 'head'), may hold values from -0.125 to 0.125
- w_value: bfloat16 [2048, 2048], P('seq', 'head'), may hold values from -0.125 to 0.125
- w_out: bfloat16 [2048, 2048], P('head', 'seq'), may hold values from -0.125 to 0.125
Outputs:
- cross_out: bfloat16 [32768, 2048], P(('batch', 'seq'), 'head'), parts along dimension 0
The draws below stay inside these ranges and needn't reach their ends.
There are 2 independent parts, one for each index of `batch`. The reference program is written for one: setup_inputs(seed, part) draws one part's arguments, and reference() takes and returns one part's arrays. A program takes and returns all parts, laid end to end along the dimension named above; an argument that names none is the same for every part. Nothing has to cross between parts.
Inputs may be any that keep to these rules, and one draw needn't show every extreme that they name: Entry c picks row c // 16 * 16 + slots[c] of neighbor_bank.
All inputs are finite; a program needn't handle non-finite values.
Results may differ from the reference program's by a relative error of at most 0.006.
The reference program's roundings to bfloat16 on the way (of `normed`, `queries`, `retrieved`, `weights` and `attended`) count: a program that leaves them out, or rounds other values in their place, can miss the bound.
Values may be sent and summed in bfloat16 or wider, within the bound.
A program may use at most 128 MiB of HBM per device.

```python
import math
import jax
import jax.numpy as jnp
from jax import lax

D = 2048
HEADS = 16
HEAD_DIM = 128
BLOCK = 64
NEIGHBORS = 2
NEIGH_LEN = 128
BLOCK_DEV = 16
TOKENS = 16384
BLOCKS = 256


def draw_neighbor_bank(key, part):
    key_base = jax.random.fold_in(jax.random.fold_in(key, 11), 0)
    rows = NEIGHBORS * NEIGH_LEN
    base = jnp.clip(jax.random.normal(key_base, (BLOCKS, rows, D), jnp.float32) * 2.0, -8.0, 8.0)
    return base.astype(jnp.bfloat16)


def plant(drawn, own_key, low, largest):
    dims = drawn.shape
    spot = [jax.random.randint(jax.random.fold_in(own_key, axis), (), 0, dims[axis]) for axis in range(len(dims))]
    drawn = drawn.at[tuple(spot)].set(low)
    longest = dims.index(max(dims))
    spot[longest] = (spot[longest] + 1) % dims[longest]
    return drawn.at[tuple(spot)].set(largest)


def block_scale(rng, extent, cuts, smallest, high):
    def one(dim, parts):
        steps = jax.random.uniform(jax.random.fold_in(jax.random.fold_in(rng, 6), dim), (parts,), jnp.float32, smallest / len(cuts), high / len(cuts))
        return jnp.repeat(jnp.exp(steps), extent[dim] // parts).reshape((-1,) + (1,) * (len(extent) - dim - 1))

    loudness = one(*cuts[0])
    for cut in cuts[1:]:
        loudness = loudness * one(*cut)
    return loudness


def noise(key, dims, scale, reach, cuts=(), kind=jnp.bfloat16):
    entries = jax.random.normal(key, dims, jnp.float32) * scale
    if len(cuts) > 0:
        entries = block_scale(key, dims, cuts, -0.22, 0.18) * entries
    return jnp.clip(entries, min=-reach, max=reach).astype(kind)


def setup_inputs(seed: int = 0, part: int = 0) -> dict:
    streams_of = jax.random.split(jax.random.key(seed), 8)
    part_splits = jax.random.split(jax.random.fold_in(streams_of[7], part), 8)
    tokens = noise(part_splits[0], (TOKENS, D), 1.0, 6.0, ((0, 16),))
    neighbor_bank = draw_neighbor_bank(jax.random.fold_in(jax.random.fold_in(streams_of[7], part), 71), part)
    slots = plant(jax.random.randint(part_splits[2], (BLOCKS,), 0, BLOCK_DEV), jax.random.fold_in(part_splits[2], 1), 0, BLOCK_DEV - 1).astype(jnp.int32)
    w_query = noise(streams_of[3], (D, D), D ** -0.5, 0.125, ((0, 16), (1, 4)))
    w_key = noise(streams_of[4], (D, D), D ** -0.5, 0.125, ((0, 16), (1, 4)))
    w_value = noise(streams_of[5], (D, D), D ** -0.5, 0.125, ((0, 16), (1, 4)))
    w_out = noise(streams_of[6], (D, D), D ** -0.5, 0.125, ((0, 4), (1, 16)))
    return {"tokens": tokens, "neighbor_bank": neighbor_bank, "slots": slots, "w_query": w_query, "w_key": w_key, "w_value": w_value, "w_out": w_out}


def rms_normed(tokens):
    hidden = tokens.astype(jnp.float32)
    scale_row = lax.rsqrt(lax.optimization_barrier(jnp.mean(hidden * hidden, axis=-1, keepdims=True)) + 1e-06)
    return (hidden * scale_row).astype(jnp.bfloat16)

def reference(tokens, neighbor_bank, slots, w_query, w_key, w_value, w_out):
    normed = rms_normed(tokens)
    queries = jnp.dot(normed, w_query, preferred_element_type=jnp.float32).astype(jnp.bfloat16)
    block_ids = jnp.arange(BLOCKS, dtype=jnp.int32)
    bank_rows = (block_ids // BLOCK_DEV * BLOCK_DEV + slots).astype(jnp.int32)
    retrieved = jnp.take(neighbor_bank, bank_rows, axis=0).reshape(BLOCKS * NEIGHBORS * NEIGH_LEN, D)
    key_rows = jnp.dot(retrieved, w_key, preferred_element_type=jnp.float32).astype(jnp.bfloat16)
    value_rows = jnp.dot(retrieved, w_value, preferred_element_type=jnp.float32).astype(jnp.bfloat16)
    key_rows = key_rows.reshape(BLOCKS, NEIGHBORS * NEIGH_LEN, HEADS, HEAD_DIM)
    value_rows = value_rows.reshape(BLOCKS, NEIGHBORS * NEIGH_LEN, HEADS, HEAD_DIM)
    padding = jnp.zeros((1, NEIGHBORS * NEIGH_LEN, HEADS, HEAD_DIM), jnp.bfloat16)
    prior_keys = jnp.concatenate([padding, key_rows[:-1]], axis=0)
    prior_values = jnp.concatenate([padding, value_rows[:-1]], axis=0)
    query_blocks = queries.reshape(BLOCKS, BLOCK, HEADS, HEAD_DIM)
    scores = jnp.einsum('cmhd,cnhd->chmn', query_blocks.astype(jnp.float32), prior_keys.astype(jnp.float32)) / math.sqrt(HEAD_DIM)
    peak_score = lax.optimization_barrier(jnp.max(scores, axis=-1, keepdims=True))
    exponent = jnp.exp(scores - peak_score)
    weights = (exponent / lax.optimization_barrier(jnp.sum(exponent, axis=-1, keepdims=True))).astype(jnp.bfloat16)
    attended = jnp.einsum('chmn,cnhd->cmhd', weights.astype(jnp.float32), prior_values.astype(jnp.float32))
    attended = attended.astype(jnp.bfloat16).reshape(TOKENS, D)
    return jnp.dot(attended, w_out, preferred_element_type=jnp.float32).astype(jnp.bfloat16)
```

```python
import functools
import math

import jax
import jax.numpy as jnp
from jax import lax
from jax.experimental import pallas as pl
from jax.experimental.pallas import tpu as pltpu
from jax.sharding import PartitionSpec as P

MESH = pl.DeviceIdType.MESH
HEAD_DIM = 128
BLOCKS = 16
BLOCK = 64
KEYS = 256
D = 2048
ROWS = BLOCKS * BLOCK
HEADS = 4
GROUPS = 2
GROUP_ROWS = ROWS // GROUPS
SCALE = 1.0 / math.sqrt(HEAD_DIM)
BF16 = jnp.bfloat16
F32 = jnp.float32


def kernel(
    tokens,
    bank_hbm,
    slots,
    w_query,
    w_key,
    w_value,
    w_out,
    out,
    normed,
    bank,
    w_all,
    o_all,
    queries,
    kv_pairs,
    kv_send,
    kv_recv,
    attended,
    total,
    stage_sem,
    load_sem,
    w_send,
    w_recv,
    y_send,
    y_recv,
    kv_send_sem,
    kv_recv_sem,
    perm_sem,
):
    seq = lax.axis_index("seq")
    y = lax.axis_index("head")
    half = lax.axis_index("batch")
    p = lax.div(seq, 8)
    z = lax.rem(lax.div(seq, 2), 4)
    c = lax.rem(seq, 2)
    z_next = lax.rem(z + 1, 4)
    z_prev = lax.rem(z + 3, 4)
    z_far = lax.rem(z + 2, 4)

    def device(s, h, b):
        return {"seq": s, "head": h, "batch": b}

    up = device(p * 8 + z_next * 2 + c, y, half)
    down = device(p * 8 + z_prev * 2 + c, y, half)
    flip = (1 - p) * 8 + z * 2 + c
    side = device(flip, y, half)
    other_side = device(flip, y, 1 - half)
    partner = device(p * 8 + z * 2 + 1 - c, y, half)
    y_up = device(seq, lax.rem(y + 1, 4), half)
    y_down = device(seq, lax.rem(y + 3, 4), half)
    later = device(lax.rem(seq + 1, 16), y, half)
    earlier = device(lax.rem(seq + 15, 16), y, half)
    quarter = lax.div(seq, 4)
    lane = lax.rem(seq, 4)
    moves = quarter != y
    perm_seq = 4 * y + lane
    perm = device(perm_seq, quarter, half)
    y_next = lax.rem(y + 1, 4)
    y_prev = lax.rem(y + 3, 4)

    def slab(r, q, zz, cc, part=None):
        if r < HEADS:
            ref = w_all.at[r, q, zz, cc]
            rows = 128
        else:
            ref = o_all.at[q, zz, cc]
            rows = 512
        if part is None:
            return ref
        return ref.at[pl.ds(part * (rows // 2), rows // 2)]

    def sent(src, dst, ss, rs, to):
        return pltpu.make_async_remote_copy(
            src_ref=src, dst_ref=dst, send_sem=ss, recv_sem=rs, device_id=to, device_id_type=MESH
        )

    def stage(h):
        cols = pl.ds(h * HEAD_DIM, HEAD_DIM)
        return [
            pltpu.make_async_copy(
                w.at[:, cols],
                w_all.at[h, p, z, c, :, pl.ds(n * HEAD_DIM, HEAD_DIM)],
                stage_sem.at[h, n],
            )
            for n, w in enumerate((w_query, w_key, w_value))
        ]

    token_copy = pltpu.make_async_copy(tokens, normed, load_sem.at[BLOCKS])
    bank_copies = [pltpu.make_async_copy(bank_hbm.at[b], bank.at[b], load_sem.at[b]) for b in range(BLOCKS)]
    perm_local = pltpu.make_async_copy(w_out, o_all.at[p, z, c], load_sem.at[BLOCKS + 1])
    perm_dst = o_all.at[lax.div(perm_seq, 8), lax.rem(lax.div(perm_seq, 2), 4), lax.rem(perm_seq, 2)]
    perm_copy = sent(w_out, perm_dst, perm_sem.at[0], perm_sem.at[1], perm)

    for copy in stage(0) + stage(1):
        copy.start()
    token_copy.start()
    for copy in stage(2) + stage(3):
        copy.start()
    for copy in bank_copies:
        copy.start()

    barrier = pltpu.get_barrier_semaphore()
    for peer in (up, down, side, other_side, partner, y_up, y_down, later, earlier):
        pl.semaphore_signal(barrier, inc=1, device_id=peer, device_id_type=MESH)

    @pl.when(moves)
    def _():
        pl.semaphore_signal(barrier, inc=1, device_id=perm, device_id_type=MESH)

    pl.semaphore_wait(barrier, 9 + moves.astype(jnp.int32))

    def w_copy(r, k):
        own = (p, z, c)
        before, after, far = (p, z_prev, c), (p, z_next, c), (p, z_far, c)
        where, part, to = {
            0: (own, None, up),
            1: (own, None, down),
            2: (before, 0, up),
            3: (after, 1, down),
            4: (own, 0, side),
            5: (own, 1, other_side),
            6: (before, 0, side),
            7: (before, 1, other_side),
            8: (after, 0, side),
            9: (after, 1, other_side),
            10: (far, 0, side),
            11: (far, 1, other_side),
            12: (own, None, partner),
            13: (before, None, partner),
            14: (after, None, partner),
            15: (far, None, partner),
        }[k]
        ref = slab(r, *where, part)
        return sent(ref, ref, w_send.at[r, k], w_recv.at[r, k], to)

    def w_far_side(r):
        ref = w_all.at[r, 1 - p, :, c] if r < HEADS else o_all.at[1 - p, :, c]
        return sent(ref, ref, w_send.at[r, 16], w_recv.at[r, 16], partner)

    def begin(r):
        if r < HEADS:
            for copy in stage(r):
                copy.wait()
        else:

            @pl.when(moves)
            def _():
                perm_copy.wait_recv()

            @pl.when(jnp.logical_not(moves))
            def _():
                perm_local.wait()

        for k in (0, 1, 4, 5, 12):
            w_copy(r, k).start()

    def relay(r):
        w_copy(r, 0).wait_recv()
        for k in (2, 6, 7, 13):
            w_copy(r, k).start()
        w_copy(r, 1).wait_recv()
        for k in (3, 8, 9, 14):
            w_copy(r, k).start()

    def relay_far(r):
        w_copy(r, 2).wait_recv()
        w_copy(r, 10).start()
        w_copy(r, 3).wait_recv()
        w_copy(r, 11).start()
        w_copy(r, 15).start()

    def cross(r):
        for k in range(4, 12):
            w_copy(r, k).wait_recv()
        w_far_side(r).start()

    def arrived(r):
        for k in range(12, 16):
            w_copy(r, k).wait_recv()
        w_far_side(r).wait_recv()

    def y_copy(h, g, k):
        n = h * GROUPS + g
        whose, part, to = {
            0: (y, None, y_up),
            1: (y, None, y_down),
            2: (y_prev, 0, y_up),
            3: (y_next, 1, y_down),
        }[k]
        if part is None:
            rows = pl.ds(g * GROUP_ROWS, GROUP_ROWS)
        else:
            rows = pl.ds(g * GROUP_ROWS + part * (GROUP_ROWS // 2), GROUP_ROWS // 2)
        ref = attended.at[h, whose, rows]
        return sent(ref, ref, y_send.at[n, k], y_recv.at[n, k], to)

    def share(n):
        for k in (0, 1):
            y_copy(n // GROUPS, n % GROUPS, k).start()

    def share_relay(n):
        h, g = n // GROUPS, n % GROUPS
        y_copy(h, g, 0).wait_recv()
        y_copy(h, g, 2).start()
        y_copy(h, g, 1).wait_recv()
        y_copy(h, g, 3).start()

    def share_done(n):
        for k in (2, 3):
            y_copy(n // GROUPS, n % GROUPS, k).wait_recv()

    def kv_hand(h):
        return sent(kv_send.at[h], kv_recv.at[h], kv_send_sem.at[h], kv_recv_sem.at[h], later)

    def normalize():
        def body(i, carry):
            rows = pl.ds(pl.multiple_of(i * 64, 64), 64)
            hidden = normed[rows, :].astype(F32)
            scale = lax.rsqrt(jnp.mean(hidden * hidden, axis=-1, keepdims=True) + 1e-06)
            normed[rows, :] = (hidden * scale).astype(BF16)
            return carry

        lax.fori_loop(0, ROWS // 64, body, 0)

    def weights(h, start, width):
        return w_all[h, :, :, :, :, pl.ds(start, width)].reshape(D, width)

    def project_queries(h):
        def body(i, carry):
            rows = pl.ds(pl.multiple_of(i * 256, 256), 256)
            queries[h % 2, rows, :] = jnp.dot(
                normed[rows, :], weights(h, 0, HEAD_DIM), preferred_element_type=F32
            ).astype(BF16)
            return carry

        lax.fori_loop(0, ROWS // 256, body, 0)

    def project_pair(h, first, second):
        rows = jnp.concatenate([bank[slots[first]], bank[slots[second]]], axis=0)
        return jnp.dot(rows, weights(h, HEAD_DIM, 2 * HEAD_DIM), preferred_element_type=F32).astype(BF16)

    def attend(h, position, keys, values, first=False):
        block = 0 if first else position + 1
        row = block * BLOCK
        if not isinstance(row, int):
            row = pl.multiple_of(row, BLOCK)
        q = queries[h % 2, pl.ds(row, BLOCK), :]
        scores = lax.dot_general(q, keys, (((1,), (1,)), ((), ())), preferred_element_type=F32) * SCALE
        peak = jnp.max(scores, axis=-1, keepdims=True)
        exponent = jnp.exp(scores - peak)
        inverse = 1.0 / jnp.sum(exponent, axis=-1, keepdims=True)
        probs = (exponent * inverse).astype(BF16)
        mixed = jnp.dot(probs, values, preferred_element_type=F32)
        if first:
            mixed = jnp.where(seq == 0, jnp.zeros_like(mixed), mixed)
        at = position * BLOCK
        if not isinstance(at, int):
            at = pl.multiple_of(at, BLOCK)
        attended[h, y, pl.ds(at, BLOCK), :] = mixed.astype(BF16)

    def from_pair(parity, which):
        rows = pl.ds(which * KEYS, KEYS)
        return kv_pairs[parity, rows, 0:HEAD_DIM], kv_pairs[parity, rows, HEAD_DIM : 2 * HEAD_DIM]

    def from_earlier(h):
        return kv_recv[h, :, 0:HEAD_DIM], kv_recv[h, :, HEAD_DIM : 2 * HEAD_DIM]

    def step(h, i, parity):
        if isinstance(i, int) and i == 0:
            if h > 0:
                attend(h - 1, 13, *from_pair(1, 0))
                attend(h - 1, 14, *from_pair(1, 1))
            pair = project_pair(h, 15, 0)
            kv_send[h] = pair[0:KEYS]
            kv_pairs[0, KEYS : 2 * KEYS, :] = pair[KEYS : 2 * KEYS]
            return
        if isinstance(i, int) and i == 1:
            if h > 0:
                kv_hand(h - 1).wait_recv()
                attend(h - 1, 15, *from_earlier(h - 1), first=True)
            attend(h, 0, *from_pair(0, 1))
        else:
            attend(h, 2 * i - 3, *from_pair(1 - parity, 0))
            attend(h, 2 * i - 2, *from_pair(1 - parity, 1))
        kv_pairs[parity] = project_pair(h, 2 * i - 1, 2 * i)

    def out_weights(h):
        rows = pl.ds(h * 128, 128)
        return jnp.concatenate(
            [
                jnp.concatenate([o_all[t // 8, (t // 2) % 4, t % 2, rows, :] for t in range(4 * g, 4 * g + 4)], axis=1)
                for g in range(4)
            ],
            axis=0,
        )

    def project_out(n):
        h, g = n // GROUPS, n % GROUPS
        rows = pl.ds(g * GROUP_ROWS, GROUP_ROWS)
        wide = jnp.concatenate([attended[h, g2, rows, :] for g2 in range(4)], axis=1)
        added = jnp.dot(wide, out_weights(h), preferred_element_type=F32)
        if h == 0:
            total[rows, :] = added
        elif h < HEADS - 1:
            total[rows, :] += added
        else:
            done = (total[rows, :] + added).astype(BF16)
            start = g * GROUP_ROWS + BLOCK
            if g < GROUPS - 1:
                out[start : start + GROUP_ROWS, :] = done
            else:
                out[start:ROWS, :] = done[: GROUP_ROWS - BLOCK]
                out[0:BLOCK, :] = done[GROUP_ROWS - BLOCK :]

    begin(0)

    @pl.when(moves)
    def _():
        perm_copy.start()

    @pl.when(jnp.logical_not(moves))
    def _():
        perm_local.start()

    begin(1)
    token_copy.wait()
    normalize()
    relay(0)
    relay_far(0)
    relay(1)
    cross(0)
    for copy in bank_copies:
        copy.wait()
    arrived(0)

    after = {
        (0, 0): [lambda: relay_far(1), lambda: begin(2)],
        (0, 3): [lambda: cross(1), lambda: relay(2)],
        (0, 5): [lambda: relay_far(2), lambda: begin(3), lambda: share(0)],
        (0, 7): [lambda: cross(2), lambda: arrived(1)],
        (1, 0): [lambda: relay(3)],
        (1, 1): [lambda: relay_far(3), lambda: begin(4), lambda: share(1)],
        (1, 3): [lambda: cross(3), lambda: relay(4)],
        (1, 5): [lambda: relay_far(4), lambda: share_relay(0), lambda: share(2)],
        (1, 7): [lambda: arrived(2)],
        (2, 1): [lambda: share(3), lambda: share_relay(1), lambda: cross(4)],
        (2, 5): [lambda: share_relay(2), lambda: share(4)],
        (2, 7): [lambda: arrived(3)],
        (3, 1): [lambda: share(5), lambda: share_relay(3), lambda: arrived(4)],
        (3, 5): [lambda: share(6)],
        (3, 7): [lambda: share_relay(4)],
    }

    def ticks(h, i):
        for f in after.get((h, i), ()):
            f()

    for h in range(HEADS):
        project_queries(h)
        step(h, 0, 0)
        ticks(h, 0)
        step(h, 1, 1)
        kv_hand(h).start()
        ticks(h, 1)
        for stretch in ((2, 4), (4, 6), (6, 8)):
            step(h, stretch[0], 0)
            step(h, stretch[0] + 1, 1)
            ticks(h, stretch[1] - 1)

    last = HEADS - 1
    attend(last, 13, *from_pair(1, 0))
    attend(last, 14, *from_pair(1, 1))
    kv_hand(last).wait_recv()
    attend(last, 15, *from_earlier(last), first=True)
    share_done(0)
    project_out(0)
    share(7)
    share_done(1)
    project_out(1)
    share_relay(5)
    share_done(2)
    project_out(2)
    share_done(3)
    project_out(3)
    share_relay(6)
    share_done(4)
    project_out(4)
    share_relay(7)
    share_done(5)
    project_out(5)
    share_done(6)
    project_out(6)
    share_done(7)
    project_out(7)

    for r in range(HEADS + 1):
        for k in range(16):
            w_copy(r, k).wait_send()
        w_far_side(r).wait_send()
    for n in range(HEADS * GROUPS):
        for k in range(4):
            y_copy(n // GROUPS, n % GROUPS, k).wait_send()
    for h in range(HEADS):
        kv_hand(h).wait_send()

    @pl.when(moves)
    def _():
        perm_copy.wait_send()


def local(tokens, neighbor_bank, slots, w_query, w_key, w_value, w_out):
    hbm = pl.BlockSpec(memory_space=pl.ANY)
    return pl.pallas_call(
        kernel,
        out_shape=jax.ShapeDtypeStruct((ROWS, HEADS * HEAD_DIM), BF16),
        in_specs=[hbm, hbm, pl.BlockSpec(memory_space=pltpu.SMEM), hbm, hbm, hbm, hbm],
        out_specs=pl.BlockSpec(memory_space=pltpu.VMEM),
        scratch_shapes=[
            pltpu.VMEM((ROWS, D), BF16),
            pltpu.VMEM((BLOCKS, KEYS, D), BF16),
            pltpu.VMEM((HEADS, 2, 4, 2, 128, 3 * HEAD_DIM), BF16),
            pltpu.VMEM((2, 4, 2, 512, 128), BF16),
            pltpu.VMEM((2, ROWS, HEAD_DIM), BF16),
            pltpu.VMEM((2, 2 * KEYS, 2 * HEAD_DIM), BF16),
            pltpu.VMEM((HEADS, KEYS, 2 * HEAD_DIM), BF16),
            pltpu.VMEM((HEADS, KEYS, 2 * HEAD_DIM), BF16),
            pltpu.VMEM((HEADS, 4, ROWS, HEAD_DIM), BF16),
            pltpu.VMEM((ROWS, 512), F32),
            pltpu.SemaphoreType.DMA((HEADS, 3)),
            pltpu.SemaphoreType.DMA((BLOCKS + 2,)),
            pltpu.SemaphoreType.DMA((HEADS + 1, 17)),
            pltpu.SemaphoreType.DMA((HEADS + 1, 17)),
            pltpu.SemaphoreType.DMA((HEADS * GROUPS, 4)),
            pltpu.SemaphoreType.DMA((HEADS * GROUPS, 4)),
            pltpu.SemaphoreType.DMA((HEADS,)),
            pltpu.SemaphoreType.DMA((HEADS,)),
            pltpu.SemaphoreType.DMA((2,)),
        ],
        compiler_params=pltpu.CompilerParams(
            collective_id=0, has_side_effects=True, vmem_limit_bytes=64 * 1024 * 1024 - 512 * 1024
        ),
        name="attention",
    )(tokens, neighbor_bank, slots, w_query, w_key, w_value, w_out)


def solution(mesh):
    in_specs = (
        P(("batch", "seq"), None),
        P(("batch", "seq"), None, None),
        P(("batch", "seq")),
        P("seq", "head"),
        P("seq", "head"),
        P("seq", "head"),
        P("head", "seq"),
    )
    out_specs = P(("batch", "seq"), "head")
    return jax.shard_map(local, mesh=mesh, in_specs=in_specs, out_specs=out_specs, check_vma=False)
```

```python
import functools
import math

import jax
import jax.numpy as jnp
from jax import lax
from jax.experimental import pallas as pl
from jax.experimental.pallas import tpu as pltpu
from jax.sharding import PartitionSpec as P

MESH = pl.DeviceIdType.MESH
HEAD_DIM = 128
BLOCKS = 16
BLOCK = 64
KEYS = 256
D = 2048
ROWS = BLOCKS * BLOCK
HEADS = 4
GROUPS = 2
GROUP_ROWS = ROWS // GROUPS
WIDTH = 2 * HEAD_DIM
KV_ROUND = (0, 2, 3, 5)
Q_ROUND = (1, 4)
O_ROUND = 6
KV_IN = 2 * BLOCKS
KV_OUT = KV_IN + HEADS + 1
SCALE = 1.0 / math.sqrt(HEAD_DIM)
BF16 = jnp.bfloat16
F32 = jnp.float32


def kernel(
    tokens,
    bank_hbm,
    slots,
    w_query,
    w_key,
    w_value,
    w_out,
    out,
    normed,
    bank,
    w_all,
    o_all,
    queries,
    kv,
    attended,
    total,
    stage_sem,
    load_sem,
    w_send,
    w_recv,
    y_send,
    y_recv,
    kv_send_sem,
    kv_recv_sem,
    perm_sem,
):
    seq = lax.axis_index("seq")
    y = lax.axis_index("head")
    half = lax.axis_index("batch")
    p = lax.div(seq, 8)
    z = lax.rem(lax.div(seq, 2), 4)
    c = lax.rem(seq, 2)
    z_next = lax.rem(z + 1, 4)
    z_prev = lax.rem(z + 3, 4)
    z_far = lax.rem(z + 2, 4)

    def device(s, h, b):
        return {"seq": s, "head": h, "batch": b}

    up = device(p * 8 + z_next * 2 + c, y, half)
    down = device(p * 8 + z_prev * 2 + c, y, half)
    flip = (1 - p) * 8 + z * 2 + c
    side = device(flip, y, half)
    other_side = device(flip, y, 1 - half)
    partner = device(p * 8 + z * 2 + 1 - c, y, half)
    y_up = device(seq, lax.rem(y + 1, 4), half)
    y_down = device(seq, lax.rem(y + 3, 4), half)
    later = device(lax.rem(seq + 1, 16), y, half)
    earlier = device(lax.rem(seq + 15, 16), y, half)
    quarter = lax.div(seq, 4)
    lane = lax.rem(seq, 4)
    moves = quarter != y
    perm_seq = 4 * y + lane
    perm = device(perm_seq, quarter, half)
    y_next = lax.rem(y + 1, 4)
    y_prev = lax.rem(y + 3, 4)

    def slab(r, q, zz, cc, part=None):
        if r < O_ROUND:
            ref = w_all.at[r, q, zz, cc]
            rows = 128
        else:
            ref = o_all.at[q, zz, cc]
            rows = 512
        if part is None:
            return ref
        return ref.at[pl.ds(part * (rows // 2), rows // 2)]

    def sent(src, dst, ss, rs, to):
        return pltpu.make_async_remote_copy(
            src_ref=src, dst_ref=dst, send_sem=ss, recv_sem=rs, device_id=to, device_id_type=MESH
        )

    def stage(r):
        if r in Q_ROUND:
            parts = [(w_query, Q_ROUND.index(r) * WIDTH, 0, WIDTH)]
        else:
            h = KV_ROUND.index(r)
            parts = [(w_key, h * HEAD_DIM, 0, HEAD_DIM), (w_value, h * HEAD_DIM, HEAD_DIM, HEAD_DIM)]
        return [
            pltpu.make_async_copy(
                w.at[:, pl.ds(start, width)], w_all.at[r, p, z, c, :, pl.ds(at, width)], stage_sem.at[r, n]
            )
            for n, (w, start, at, width) in enumerate(parts)
        ]

    token_copy = pltpu.make_async_copy(tokens, normed, load_sem.at[BLOCKS])
    bank_copies = [pltpu.make_async_copy(bank_hbm.at[b], bank.at[b], load_sem.at[b]) for b in range(BLOCKS)]
    perm_local = pltpu.make_async_copy(w_out, o_all.at[p, z, c], load_sem.at[BLOCKS + 1])
    perm_dst = o_all.at[lax.div(perm_seq, 8), lax.rem(lax.div(perm_seq, 2), 4), lax.rem(perm_seq, 2)]
    perm_copy = sent(w_out, perm_dst, perm_sem.at[0], perm_sem.at[1], perm)

    barrier = pltpu.get_barrier_semaphore()
    for peer in (up, down, side, other_side, partner, y_up, y_down, later, earlier):
        pl.semaphore_signal(barrier, inc=1, device_id=peer, device_id_type=MESH)

    @pl.when(moves)
    def _():
        pl.semaphore_signal(barrier, inc=1, device_id=perm, device_id_type=MESH)

    for r in range(O_ROUND):
        for copy in stage(r):
            copy.start()
        if r == 1:
            token_copy.start()

    pl.semaphore_wait(barrier, 9 + moves.astype(jnp.int32))

    def w_copy(r, k):
        own = (p, z, c)
        before, after, far = (p, z_prev, c), (p, z_next, c), (p, z_far, c)
        where, part, to = {
            0: (own, None, up),
            1: (own, None, down),
            2: (before, 0, up),
            3: (after, 1, down),
            4: (own, 0, side),
            5: (own, 1, other_side),
            6: (before, 0, side),
            7: (before, 1, other_side),
            8: (after, 0, side),
            9: (after, 1, other_side),
            10: (far, 0, side),
            11: (far, 1, other_side),
            12: (own, None, partner),
            13: (before, None, partner),
            14: (after, None, partner),
            15: (far, None, partner),
        }[k]
        ref = slab(r, *where, part)
        return sent(ref, ref, w_send.at[r, k], w_recv.at[r, k], to)

    def w_far_side(r):
        ref = w_all.at[r, 1 - p, :, c] if r < O_ROUND else o_all.at[1 - p, :, c]
        return sent(ref, ref, w_send.at[r, 16], w_recv.at[r, 16], partner)

    def begin(r):
        if r < O_ROUND:
            for copy in stage(r):
                copy.wait()
        else:

            @pl.when(moves)
            def _():
                perm_copy.wait_recv()

            @pl.when(jnp.logical_not(moves))
            def _():
                perm_local.wait()

        for k in (0, 1, 4, 5, 12):
            w_copy(r, k).start()

    def relay(r):
        w_copy(r, 0).wait_recv()
        for k in (2, 6, 7, 13):
            w_copy(r, k).start()
        w_copy(r, 1).wait_recv()
        for k in (3, 8, 9, 14):
            w_copy(r, k).start()

    def relay_far(r):
        w_copy(r, 2).wait_recv()
        w_copy(r, 10).start()
        w_copy(r, 3).wait_recv()
        w_copy(r, 11).start()
        w_copy(r, 15).start()

    def cross(r):
        for k in range(4, 12):
            w_copy(r, k).wait_recv()
        w_far_side(r).start()

    def arrived(r):
        for k in range(12, 16):
            w_copy(r, k).wait_recv()
        w_far_side(r).wait_recv()

    def y_copy(h, g, k):
        n = h * GROUPS + g
        whose, part, to = {
            0: (y, None, y_up),
            1: (y, None, y_down),
            2: (y_prev, 0, y_up),
            3: (y_next, 1, y_down),
        }[k]
        if part is None:
            rows = pl.ds(g * GROUP_ROWS, GROUP_ROWS)
        else:
            rows = pl.ds(g * GROUP_ROWS + part * (GROUP_ROWS // 2), GROUP_ROWS // 2)
        ref = attended.at[h + 1, whose, rows]
        return sent(ref, ref, y_send.at[n, k], y_recv.at[n, k], to)

    def share(n):
        for k in (0, 1):
            y_copy(n // GROUPS, n % GROUPS, k).start()

    def share_relay(n):
        h, g = n // GROUPS, n % GROUPS
        y_copy(h, g, 0).wait_recv()
        y_copy(h, g, 2).start()
        y_copy(h, g, 1).wait_recv()
        y_copy(h, g, 3).start()

    def share_done(n):
        for k in (2, 3):
            y_copy(n // GROUPS, n % GROUPS, k).wait_recv()

    def kv_hand(h):
        return sent(kv.at[KV_OUT + h], kv.at[KV_IN + h + 1], kv_send_sem.at[h], kv_recv_sem.at[h], later)

    def normalize():
        def body(i, carry):
            rows = pl.ds(pl.multiple_of(i * 64, 64), 64)
            hidden = normed[rows, :].astype(F32)
            scale = lax.rsqrt(jnp.mean(hidden * hidden, axis=-1, keepdims=True) + 1e-06)
            normed[rows, :] = (hidden * scale).astype(BF16)
            return carry

        lax.fori_loop(0, ROWS // 64, body, 0)

    def weights(r):
        return w_all[r].reshape(D, WIDTH)

    def project_queries(pair):
        both = jnp.dot(normed[...], weights(1 + 3 * pair), preferred_element_type=F32).astype(BF16)
        queries[2 * pair + 1] = both[:, 0:HEAD_DIM]
        queries[2 * pair + 2] = both[:, HEAD_DIM:WIDTH]

    def place(task):
        return lax.div(task, BLOCKS), lax.rem(task, BLOCKS)

    def scores_of(tasks):
        scores, values = [], []
        for task in tasks:
            slot, position = place(task)
            handed = lax.div(position, BLOCKS - 1)
            rows = kv[handed * (KV_IN + slot) + (1 - handed) * (lax.rem(slot, 2) * BLOCKS + position)]
            block = lax.rem(position + 1, BLOCKS)
            q = queries[slot, pl.ds(pl.multiple_of(block * BLOCK, BLOCK), BLOCK), :]
            scores.append(
                lax.dot_general(q, rows[:, 0:HEAD_DIM], (((1,), (1,)), ((), ())), preferred_element_type=F32) * SCALE
            )
            values.append(rows[:, HEAD_DIM:WIDTH])
        return scores, values

    def probs_of(scores):
        joined = jnp.concatenate(scores, axis=0)
        exponent = jnp.exp(joined - jnp.max(joined, axis=-1, keepdims=True))
        inverse = 1.0 / jnp.sum(exponent, axis=-1, keepdims=True)
        probs = (exponent * inverse).astype(BF16)
        return [probs[n * BLOCK : (n + 1) * BLOCK] for n in range(len(scores))]

    def mix(tasks, probs, values):
        mixed = []
        for task, weight, rows in zip(tasks, probs, values):
            one = jnp.dot(weight, rows, preferred_element_type=F32)
            empty = jnp.logical_and(lax.rem(task, BLOCKS) == BLOCKS - 1, seq == 0)
            mixed.append(jnp.where(empty, jnp.zeros_like(one), one).astype(BF16))
        return mixed

    def keep(tasks, mixed):
        for task, rows in zip(tasks, mixed):
            slot, position = place(task)
            attended[slot, y, pl.ds(pl.multiple_of(position * BLOCK, BLOCK), BLOCK), :] = rows

    def attend(tasks):
        scores, values = scores_of(tasks)
        keep(tasks, mix(tasks, probs_of(scores), values))

    def step(h, i):
        n = 8 * h + i
        tasks = [2 * n + 13, 2 * n + 14]
        scores, values = scores_of(tasks)
        probs = probs_of(scores)
        first, second = lax.rem(2 * i + 15, BLOCKS), 2 * i
        rows = jnp.concatenate([bank[slots[first]], bank[slots[second]]], axis=0)
        pair = jnp.dot(rows, weights(h + lax.div(h + 1, 2)), preferred_element_type=F32).astype(BF16)
        mixed = mix(tasks, probs, values)
        own = lax.rem(h + 1, 2) * BLOCKS
        later_step = lax.div(i + 7, 8)
        kv[(1 - later_step) * (KV_OUT + h) + later_step * (own + first)] = pair[0:KEYS]
        kv[own + second] = pair[KEYS : 2 * KEYS]
        keep(tasks, mixed)

    def out_weights(h):
        rows = pl.ds(h * 128, 128)
        return jnp.concatenate(
            [
                jnp.concatenate([o_all[t // 8, (t // 2) % 4, t % 2, rows, :] for t in range(4 * g, 4 * g + 4)], axis=1)
                for g in range(4)
            ],
            axis=0,
        )

    def project_out(n):
        h, g = n // GROUPS, n % GROUPS
        rows = pl.ds(g * GROUP_ROWS, GROUP_ROWS)
        wide = jnp.concatenate([attended[h + 1, g2, rows, :] for g2 in range(4)], axis=1)
        added = jnp.dot(wide, out_weights(h), preferred_element_type=F32)
        if h == 0:
            total[rows, :] = added
        elif h < HEADS - 1:
            total[rows, :] += added
        else:
            done = (total[rows, :] + added).astype(BF16)
            start = g * GROUP_ROWS + BLOCK
            if g < GROUPS - 1:
                out[start : start + GROUP_ROWS, :] = done
            else:
                out[start:ROWS, :] = done[: GROUP_ROWS - BLOCK]
                out[0:BLOCK, :] = done[GROUP_ROWS - BLOCK :]

    def swap_out_weights():
        @pl.when(moves)
        def _():
            perm_copy.start()

        @pl.when(jnp.logical_not(moves))
        def _():
            perm_local.start()

    def load_bank():
        for copy in bank_copies:
            copy.start()

    def catch_up():
        attend([BLOCKS + n for n in range(7)])

    begin(0)
    token_copy.wait()
    normalize()
    relay(0)
    load_bank()
    begin(1)
    relay_far(0)
    relay(1)
    cross(0)
    for copy in bank_copies:
        copy.wait()
    arrived(0)

    after = {
        (0, 0): [(relay_far, 1), (begin, 2)],
        (0, 1): [(swap_out_weights,)],
        (0, 2): [(relay, 2)],
        (0, 3): [(cross, 1)],
        (0, 4): [(arrived, 1), (project_queries, 0), (catch_up,), (relay_far, 2), (begin, 3)],
        (0, 5): [(share, 0)],
        (0, 6): [(cross, 2), (relay, 3)],
        (0, 7): [(arrived, 2), (begin, 4)],
        (1, 0): [(relay_far, 3)],
        (1, 1): [(relay, 4), (begin, 5), (share, 1)],
        (1, 2): [(cross, 3)],
        (1, 3): [(relay_far, 4), (share_relay, 0)],
        (1, 4): [(relay, 5), (cross, 4), (begin, 6)],
        (1, 5): [(share, 2)],
        (1, 6): [(relay_far, 5)],
        (1, 7): [(arrived, 3), (arrived, 4), (share_relay, 1), (project_queries, 1)],
        (2, 0): [(cross, 5), (relay, 6)],
        (2, 1): [(share, 3)],
        (2, 2): [(relay_far, 6)],
        (2, 3): [(arrived, 5), (share_relay, 2)],
        (2, 4): [(cross, 6)],
        (2, 5): [(share, 4)],
        (2, 7): [(share_relay, 3)],
        (3, 1): [(share, 5)],
        (3, 5): [(share_relay, 4), (share, 6)],
        (3, 7): [(arrived, 6)],
    }

    def one_step(n, carry):
        h, i = lax.div(n, 8), lax.rem(n, 8)
        step(h, i)

        @pl.when(i == 1)
        def _():
            kv_hand(h).start()

        @pl.when(jnp.logical_and(i == 0, h > 0))
        def _():
            kv_hand(h - 1).wait_recv()

        for head in range(HEADS):

            @pl.when(h == head)
            def _(head=head):
                for (at, place_in), actions in after.items():
                    if at == head:

                        @pl.when(i == place_in)
                        def _(actions=actions):
                            for action, *rest in actions:
                                action(*rest)

        return carry

    lax.fori_loop(0, 8 * HEADS, one_step, 0)

    kv_hand(HEADS - 1).wait_recv()
    attend([BLOCKS * HEADS + n for n in (13, 14, 15)])
    share_done(0)
    project_out(0)
    share(7)
    share_done(1)
    project_out(1)
    share_relay(5)
    share_done(2)
    project_out(2)
    share_done(3)
    project_out(3)
    share_relay(6)
    share_done(4)
    project_out(4)
    share_relay(7)
    share_done(5)
    project_out(5)
    share_done(6)
    project_out(6)
    share_done(7)
    project_out(7)

    for r in range(O_ROUND + 1):
        for k in range(16):
            w_copy(r, k).wait_send()
        w_far_side(r).wait_send()
    for n in range(HEADS * GROUPS):
        for k in range(4):
            y_copy(n // GROUPS, n % GROUPS, k).wait_send()
    for h in range(HEADS):
        kv_hand(h).wait_send()

    @pl.when(moves)
    def _():
        perm_copy.wait_send()


def local(tokens, neighbor_bank, slots, w_query, w_key, w_value, w_out):
    hbm = pl.BlockSpec(memory_space=pl.ANY)
    return pl.pallas_call(
        kernel,
        out_shape=jax.ShapeDtypeStruct((ROWS, HEADS * HEAD_DIM), BF16),
        in_specs=[hbm, hbm, pl.BlockSpec(memory_space=pltpu.SMEM), hbm, hbm, hbm, hbm],
        out_specs=pl.BlockSpec(memory_space=pltpu.VMEM),
        scratch_shapes=[
            pltpu.VMEM((ROWS, D), BF16),
            pltpu.VMEM((BLOCKS, KEYS, D), BF16),
            pltpu.VMEM((O_ROUND, 2, 4, 2, 128, WIDTH), BF16),
            pltpu.VMEM((2, 4, 2, 512, 128), BF16),
            pltpu.VMEM((HEADS + 1, ROWS, HEAD_DIM), BF16),
            pltpu.VMEM((KV_OUT + HEADS, KEYS, WIDTH), BF16),
            pltpu.VMEM((HEADS + 1, 4, ROWS, HEAD_DIM), BF16),
            pltpu.VMEM((ROWS, 512), F32),
            pltpu.SemaphoreType.DMA((O_ROUND, 2)),
            pltpu.SemaphoreType.DMA((BLOCKS + 2,)),
            pltpu.SemaphoreType.DMA((O_ROUND + 1, 17)),
            pltpu.SemaphoreType.DMA((O_ROUND + 1, 17)),
            pltpu.SemaphoreType.DMA((HEADS * GROUPS, 4)),
            pltpu.SemaphoreType.DMA((HEADS * GROUPS, 4)),
            pltpu.SemaphoreType.DMA((HEADS,)),
            pltpu.SemaphoreType.DMA((HEADS,)),
            pltpu.SemaphoreType.DMA((2,)),
        ],
        compiler_params=pltpu.CompilerParams(
            collective_id=0, has_side_effects=True, vmem_limit_bytes=64 * 1024 * 1024 - 512 * 1024
        ),
        name="attention",
    )(tokens, neighbor_bank, slots, w_query, w_key, w_value, w_out)


def solution(mesh):
    in_specs = (
        P(("batch", "seq"), None),
        P(("batch", "seq"), None, None),
        P(("batch", "seq")),
        P("seq", "head"),
        P("seq", "head"),
        P("seq", "head"),
        P("head", "seq"),
    )
    out_specs = P(("batch", "seq"), "head")
    return jax.shard_map(local, mesh=mesh, in_specs=in_specs, out_specs=out_specs, check_vma=False)
```

```python
import functools
import math

import jax
import jax.numpy as jnp
from jax import lax
from jax.experimental import pallas as pl
from jax.experimental.pallas import tpu as pltpu
from jax.sharding import PartitionSpec as P

MESH = pl.DeviceIdType.MESH
HEAD_DIM = 128
BLOCKS = 16
BLOCK = 64
KEYS = 256
D = 2048
ROWS = BLOCKS * BLOCK
HEADS = 4
PIECES = (
    (0, 0, 256),
    (0, 256, 256),
    (0, 512, 512),
    (1, 0, 512),
    (1, 512, 512),
    (2, 0, 512),
    (2, 512, 512),
    (3, 0, 512),
    (3, 512, 256),
    (3, 768, 256),
)
WIDTH = 2 * HEAD_DIM
KV_ROUND = (0, 2, 3, 5)
Q_ROUND = (1, 4)
O_ROUND = 6
KV_IN = 2 * BLOCKS
KV_OUT = KV_IN + HEADS + 1
SCALE = 1.0 / math.sqrt(HEAD_DIM)
BF16 = jnp.bfloat16
F32 = jnp.float32


def kernel(
    tokens,
    bank_hbm,
    slots,
    w_query,
    w_key,
    w_value,
    w_out,
    out,
    normed,
    bank,
    w_all,
    o_all,
    queries,
    kv,
    attended,
    total,
    stage_sem,
    load_sem,
    w_send,
    w_recv,
    y_send,
    y_recv,
    kv_send_sem,
    kv_recv_sem,
    perm_sem,
):
    seq = lax.axis_index("seq")
    y = lax.axis_index("head")
    half = lax.axis_index("batch")
    p = lax.div(seq, 8)
    z = lax.rem(lax.div(seq, 2), 4)
    c = lax.rem(seq, 2)
    z_next = lax.rem(z + 1, 4)
    z_prev = lax.rem(z + 3, 4)
    z_far = lax.rem(z + 2, 4)

    def device(s, h, b):
        return {"seq": s, "head": h, "batch": b}

    up = device(p * 8 + z_next * 2 + c, y, half)
    down = device(p * 8 + z_prev * 2 + c, y, half)
    flip = (1 - p) * 8 + z * 2 + c
    side = device(flip, y, half)
    other_side = device(flip, y, 1 - half)
    partner = device(p * 8 + z * 2 + 1 - c, y, half)
    cross_up = (1 - p) * 8 + z_next * 2 + c
    cross_down = (1 - p) * 8 + z_prev * 2 + c
    side_up = device(cross_up, y, half)
    side_down = device(cross_down, y, half)
    other_up = device(cross_up, y, 1 - half)
    other_down = device(cross_down, y, 1 - half)
    y_up = device(seq, lax.rem(y + 1, 4), half)
    y_down = device(seq, lax.rem(y + 3, 4), half)
    later = device(lax.rem(seq + 1, 16), y, half)
    earlier = device(lax.rem(seq + 15, 16), y, half)
    quarter = lax.div(seq, 4)
    lane = lax.rem(seq, 4)
    moves = quarter != y
    perm_seq = 4 * y + lane
    perm = device(perm_seq, quarter, half)
    y_next = lax.rem(y + 1, 4)
    y_prev = lax.rem(y + 3, 4)

    def slab(r, q, zz, cc, part=None):
        if r < O_ROUND:
            ref = w_all.at[r, q, zz, cc]
            rows = 128
        else:
            ref = o_all.at[q, zz, cc]
            rows = 512
        if part is None:
            return ref
        return ref.at[pl.ds(part * (rows // 2), rows // 2)]

    def sent(src, dst, ss, rs, to):
        return pltpu.make_async_remote_copy(
            src_ref=src, dst_ref=dst, send_sem=ss, recv_sem=rs, device_id=to, device_id_type=MESH
        )

    def stage(r):
        if r in Q_ROUND:
            parts = [(w_query, Q_ROUND.index(r) * WIDTH, 0, WIDTH)]
        else:
            h = KV_ROUND.index(r)
            parts = [(w_key, h * HEAD_DIM, 0, HEAD_DIM), (w_value, h * HEAD_DIM, HEAD_DIM, HEAD_DIM)]
        return [
            pltpu.make_async_copy(
                w.at[:, pl.ds(start, width)], w_all.at[r, p, z, c, :, pl.ds(at, width)], stage_sem.at[r, n]
            )
            for n, (w, start, at, width) in enumerate(parts)
        ]

    token_copy = pltpu.make_async_copy(tokens, normed, load_sem.at[BLOCKS])
    bank_copies = [pltpu.make_async_copy(bank_hbm.at[b], bank.at[b], load_sem.at[b]) for b in range(BLOCKS)]
    perm_local = pltpu.make_async_copy(w_out, o_all.at[p, z, c], load_sem.at[BLOCKS + 1])
    perm_dst = o_all.at[lax.div(perm_seq, 8), lax.rem(lax.div(perm_seq, 2), 4), lax.rem(perm_seq, 2)]
    perm_copy = sent(w_out, perm_dst, perm_sem.at[0], perm_sem.at[1], perm)

    barrier = pltpu.get_barrier_semaphore()
    near = (up, down, side, other_side, partner, side_up, side_down, other_up, other_down)
    for peer in near + (y_up, y_down, later, earlier):
        pl.semaphore_signal(barrier, inc=1, device_id=peer, device_id_type=MESH)

    @pl.when(moves)
    def _():
        pl.semaphore_signal(barrier, inc=1, device_id=perm, device_id_type=MESH)

    for r in range(O_ROUND):
        for copy in stage(r):
            copy.start()
        if r == 1:
            token_copy.start()

    pl.semaphore_wait(barrier, 13 + moves.astype(jnp.int32))

    def w_copy(r, k):
        own = (p, z, c)
        before, after, far = (p, z_prev, c), (p, z_next, c), (p, z_far, c)
        where, part, to = {
            0: (own, None, up),
            1: (own, None, down),
            2: (before, 0, up),
            3: (after, 1, down),
            4: (own, 0, side),
            5: (own, 1, other_side),
            6: (before, 0, side),
            7: (before, 1, other_side),
            8: (after, 0, side),
            9: (after, 1, other_side),
            10: (before, 0, side_up),
            11: (after, 1, other_down),
            12: (own, None, partner),
            13: (before, None, partner),
            14: (after, None, partner),
            15: (far, None, partner),
        }[k]
        ref = slab(r, *where, part)
        return sent(ref, ref, w_send.at[r, k], w_recv.at[r, k], to)

    def w_far_side(r):
        ref = w_all.at[r, 1 - p, :, c] if r < O_ROUND else o_all.at[1 - p, :, c]
        return sent(ref, ref, w_send.at[r, 16], w_recv.at[r, 16], partner)

    def begin(r):
        if r < O_ROUND:
            for copy in stage(r):
                copy.wait()
        else:

            @pl.when(moves)
            def _():
                perm_copy.wait_recv()

            @pl.when(jnp.logical_not(moves))
            def _():
                perm_local.wait()

        for k in (0, 1, 4, 5, 12):
            w_copy(r, k).start()

    def relay(r):
        w_copy(r, 0).wait_recv()
        for k in (2, 10, 6, 7, 13):
            w_copy(r, k).start()
        w_copy(r, 1).wait_recv()
        for k in (3, 11, 8, 9, 14):
            w_copy(r, k).start()

    def relay_far(r):
        w_copy(r, 2).wait_recv()
        w_copy(r, 3).wait_recv()
        w_copy(r, 15).start()

    def cross(r):
        for k in range(4, 12):
            w_copy(r, k).wait_recv()
        w_far_side(r).start()

    def arrived(r):
        for k in range(12, 16):
            w_copy(r, k).wait_recv()
        w_far_side(r).wait_recv()

    def y_copy(n, k):
        h, start, count = PIECES[n]
        whose, part, to = {
            0: (y, None, y_up),
            1: (y, None, y_down),
            2: (y_prev, 0, y_up),
            3: (y_next, 1, y_down),
        }[k]
        rows = pl.ds(start, count) if part is None else pl.ds(start + part * (count // 2), count // 2)
        ref = attended.at[h + 1, whose, rows]
        return sent(ref, ref, y_send.at[n, k], y_recv.at[n, k], to)

    def share(n):
        for k in (0, 1):
            y_copy(n, k).start()

    def share_relay(n):
        y_copy(n, 0).wait_recv()
        y_copy(n, 2).start()
        y_copy(n, 1).wait_recv()
        y_copy(n, 3).start()

    def share_done(n):
        for k in (2, 3):
            y_copy(n, k).wait_recv()

    def kv_hand(h):
        return sent(kv.at[KV_OUT + h], kv.at[KV_IN + h + 1], kv_send_sem.at[h], kv_recv_sem.at[h], later)

    def normalize():
        def body(i, carry):
            rows = pl.ds(pl.multiple_of(i * 64, 64), 64)
            hidden = normed[rows, :].astype(F32)
            scale = lax.rsqrt(jnp.mean(hidden * hidden, axis=-1, keepdims=True) + 1e-06)
            normed[rows, :] = (hidden * scale).astype(BF16)
            return carry

        lax.fori_loop(0, ROWS // 64, body, 0)

    def weights(r):
        return w_all[r].reshape(D, WIDTH)

    def project_queries(pair):
        both = jnp.dot(normed[...], weights(1 + 3 * pair), preferred_element_type=F32).astype(BF16)
        queries[2 * pair + 1] = both[:, 0:HEAD_DIM]
        queries[2 * pair + 2] = both[:, HEAD_DIM:WIDTH]

    def place(task):
        return lax.div(task, BLOCKS), lax.rem(task, BLOCKS)

    def scores_of(tasks):
        scores, values = [], []
        for task in tasks:
            slot, position = place(task)
            handed = lax.div(position, BLOCKS - 1)
            rows = kv[handed * (KV_IN + slot) + (1 - handed) * (lax.rem(slot, 2) * BLOCKS + position)]
            block = lax.rem(position + 1, BLOCKS)
            q = queries[slot, pl.ds(pl.multiple_of(block * BLOCK, BLOCK), BLOCK), :]
            scores.append(
                lax.dot_general(q, rows[:, 0:HEAD_DIM], (((1,), (1,)), ((), ())), preferred_element_type=F32) * SCALE
            )
            values.append(rows[:, HEAD_DIM:WIDTH])
        return scores, values

    def probs_of(scores):
        joined = jnp.concatenate(scores, axis=0)
        exponent = jnp.exp(joined - jnp.max(joined, axis=-1, keepdims=True))
        inverse = 1.0 / jnp.sum(exponent, axis=-1, keepdims=True)
        probs = (exponent * inverse).astype(BF16)
        return [probs[n * BLOCK : (n + 1) * BLOCK] for n in range(len(scores))]

    def mix(tasks, probs, values):
        mixed = []
        for task, weight, rows in zip(tasks, probs, values):
            one = jnp.dot(weight, rows, preferred_element_type=F32)
            empty = jnp.logical_and(lax.rem(task, BLOCKS) == BLOCKS - 1, seq == 0)
            mixed.append(jnp.where(empty, jnp.zeros_like(one), one).astype(BF16))
        return mixed

    def keep(tasks, mixed):
        for task, rows in zip(tasks, mixed):
            slot, position = place(task)
            attended[slot, y, pl.ds(pl.multiple_of(position * BLOCK, BLOCK), BLOCK), :] = rows

    def attend(tasks):
        scores, values = scores_of(tasks)
        keep(tasks, mix(tasks, probs_of(scores), values))

    def step(h, i):
        n = 8 * h + i
        tasks = [2 * n + 13, 2 * n + 14]
        scores, values = scores_of(tasks)
        probs = probs_of(scores)
        first, second = lax.rem(2 * i + 15, BLOCKS), 2 * i
        rows = jnp.concatenate([bank[slots[first]], bank[slots[second]]], axis=0)
        pair = jnp.dot(rows, weights(h + lax.div(h + 1, 2)), preferred_element_type=F32).astype(BF16)
        mixed = mix(tasks, probs, values)
        own = lax.rem(h + 1, 2) * BLOCKS
        later_step = lax.div(i + 7, 8)
        kv[(1 - later_step) * (KV_OUT + h) + later_step * (own + first)] = pair[0:KEYS]
        kv[own + second] = pair[KEYS : 2 * KEYS]
        keep(tasks, mixed)

    def out_weights(h):
        rows = pl.ds(h * 128, 128)
        return jnp.concatenate(
            [
                jnp.concatenate([o_all[t // 8, (t // 2) % 4, t % 2, rows, :] for t in range(4 * g, 4 * g + 4)], axis=1)
                for g in range(4)
            ],
            axis=0,
        )

    def project_out(n):
        share_done(n)
        h, start, count = PIECES[n]
        rows = pl.ds(start, count)
        wide = jnp.concatenate([attended[h + 1, g, rows, :] for g in range(4)], axis=1)
        added = jnp.dot(wide, out_weights(h), preferred_element_type=F32)
        if h == 0:
            total[rows, :] = added
        elif h < HEADS - 1:
            total[rows, :] += added
        else:
            done = (total[rows, :] + added).astype(BF16)
            if start + count < ROWS:
                out[start + BLOCK : start + BLOCK + count, :] = done
            else:
                out[start + BLOCK : ROWS, :] = done[: count - BLOCK]
                out[0:BLOCK, :] = done[count - BLOCK :]

    def swap_out_weights():
        @pl.when(moves)
        def _():
            perm_copy.start()

        @pl.when(jnp.logical_not(moves))
        def _():
            perm_local.start()

    def load_bank():
        for copy in bank_copies:
            copy.start()

    def catch_up():
        attend([BLOCKS + n for n in range(7)])
        share(0)

    begin(0)
    token_copy.wait()
    normalize()
    relay(0)
    begin(1)
    begin(2)
    load_bank()
    relay_far(0)
    cross(0)
    relay(1)
    begin(3)
    for copy in bank_copies:
        copy.wait()
    arrived(0)

    after = {
        (0, 0): [(relay, 2)],
        (0, 1): [(relay_far, 1), (swap_out_weights,)],
        (0, 3): [(cross, 1), (begin, 4)],
        (0, 4): [(arrived, 1), (project_queries, 0), (catch_up,), (relay_far, 2), (relay, 3)],
        (0, 5): [(share, 1), (cross, 2)],
        (0, 6): [(begin, 5), (arrived, 2)],
        (0, 7): [(relay, 4)],
        (1, 0): [(relay_far, 3)],
        (1, 1): [(share, 2), (cross, 3), (share_relay, 0), (share_relay, 1)],
        (1, 2): [(relay, 5), (relay_far, 4)],
        (1, 3): [(arrived, 3), (begin, 6)],
        (1, 4): [(cross, 4)],
        (1, 5): [(share, 3), (relay_far, 5)],
        (1, 6): [(arrived, 4)],
        (1, 7): [(cross, 5), (project_queries, 1), (share_relay, 2)],
        (2, 0): [(relay, 6), (arrived, 5)],
        (2, 1): [(share, 4)],
        (2, 2): [(share_relay, 3)],
        (2, 4): [(relay_far, 6)],
        (2, 5): [(share, 5)],
        (2, 6): [(share_relay, 4), (cross, 6)],
        (3, 0): [(arrived, 6)],
        (3, 1): [(share, 6)],
        (3, 2): [(share_relay, 5)],
        (3, 5): [(share, 7)],
        (3, 6): [(share_relay, 6)],
        (3, 7): [(share, 8)],
    }

    def one_step(n, carry):
        h, i = lax.div(n, 8), lax.rem(n, 8)
        step(h, i)

        @pl.when(i == 1)
        def _():
            kv_hand(h).start()

        @pl.when(jnp.logical_and(i == 0, h > 0))
        def _():
            kv_hand(h - 1).wait_recv()

        for head in range(HEADS):

            @pl.when(h == head)
            def _(head=head):
                for (at, place_in), actions in after.items():
                    if at == head:

                        @pl.when(i == place_in)
                        def _(actions=actions):
                            for action, *rest in actions:
                                action(*rest)

        return carry

    lax.fori_loop(0, 8 * HEADS, one_step, 0)

    kv_hand(HEADS - 1).wait_recv()
    attend([BLOCKS * HEADS + n for n in (13, 14, 15)])
    project_out(0)
    share(9)
    project_out(1)
    project_out(2)
    share_relay(7)
    project_out(3)
    project_out(4)
    share_relay(8)
    project_out(5)
    share_relay(9)
    project_out(6)
    project_out(7)
    project_out(8)
    project_out(9)

    for r in range(O_ROUND + 1):
        for k in range(16):
            w_copy(r, k).wait_send()
        w_far_side(r).wait_send()
    for n in range(len(PIECES)):
        for k in range(4):
            y_copy(n, k).wait_send()
    for h in range(HEADS):
        kv_hand(h).wait_send()

    @pl.when(moves)
    def _():
        perm_copy.wait_send()


def local(tokens, neighbor_bank, slots, w_query, w_key, w_value, w_out):
    hbm = pl.BlockSpec(memory_space=pltpu.HBM)
    return pl.pallas_call(
        kernel,
        out_shape=jax.ShapeDtypeStruct((ROWS, HEADS * HEAD_DIM), BF16),
        in_specs=[hbm, hbm, pl.BlockSpec(memory_space=pltpu.SMEM), hbm, hbm, hbm, hbm],
        out_specs=pl.BlockSpec(memory_space=pltpu.VMEM),
        scratch_shapes=[
            pltpu.VMEM((ROWS, D), BF16),
            pltpu.VMEM((BLOCKS, KEYS, D), BF16),
            pltpu.VMEM((O_ROUND, 2, 4, 2, 128, WIDTH), BF16),
            pltpu.VMEM((2, 4, 2, 512, 128), BF16),
            pltpu.VMEM((HEADS + 1, ROWS, HEAD_DIM), BF16),
            pltpu.VMEM((KV_OUT + HEADS, KEYS, WIDTH), BF16),
            pltpu.VMEM((HEADS + 1, 4, ROWS, HEAD_DIM), BF16),
            pltpu.VMEM((ROWS, 512), F32),
            pltpu.SemaphoreType.DMA((O_ROUND, 2)),
            pltpu.SemaphoreType.DMA((BLOCKS + 2,)),
            pltpu.SemaphoreType.DMA((O_ROUND + 1, 17)),
            pltpu.SemaphoreType.DMA((O_ROUND + 1, 17)),
            pltpu.SemaphoreType.DMA((len(PIECES), 4)),
            pltpu.SemaphoreType.DMA((len(PIECES), 4)),
            pltpu.SemaphoreType.DMA((HEADS,)),
            pltpu.SemaphoreType.DMA((HEADS,)),
            pltpu.SemaphoreType.DMA((2,)),
        ],
        compiler_params=pltpu.CompilerParams(
            collective_id=0, has_side_effects=True, vmem_limit_bytes=52 * 1024 * 1024
        ),
        name="attention",
    )(*[pltpu.with_memory_space_constraint(a, pltpu.HBM) for a in (tokens, neighbor_bank, slots, w_query, w_key, w_value, w_out)])


def solution(mesh):
    in_specs = (
        P(("batch", "seq"), None),
        P(("batch", "seq"), None, None),
        P(("batch", "seq")),
        P("seq", "head"),
        P("seq", "head"),
        P("seq", "head"),
        P("head", "seq"),
    )
    out_specs = P(("batch", "seq"), "head")
    return jax.shard_map(local, mesh=mesh, in_specs=in_specs, out_specs=out_specs, check_vma=False)
```

```python
import functools
import math

import jax
import jax.numpy as jnp
from jax import lax
from jax.experimental import pallas as pl
from jax.experimental.pallas import tpu as pltpu
from jax.sharding import PartitionSpec as P

MESH = pl.DeviceIdType.MESH
HEAD_DIM = 128
BLOCKS = 16
BLOCK = 64
KEYS = 256
D = 2048
ROWS = BLOCKS * BLOCK
HEADS = 4
PIECES = tuple((h, start * BLOCK, count * BLOCK) for h in range(HEADS) for start, count in ((0, 7), (7, 4), (11, 5)))
PIECES = PIECES[:-1] + ((3, 11 * BLOCK, 3 * BLOCK), (3, 14 * BLOCK, 2 * BLOCK))
WIDTH = 2 * HEAD_DIM
KV_ROUND = (0, 2, 3, 5)
Q_ROUND = (1, 4)
O_ROUND = 6
KV_IN = 2 * BLOCKS
KV_OUT = KV_IN + HEADS + 1
SEND_OF = (0,) * 2 + (1,) * 2 + (2,) * 8 + (3,) * 5
RECV_OF = (0, 1) + (2,) * 2 + (3,) * 8 + (4,) * 5
STEP = 4
STEPS = BLOCKS // STEP
SCALE = 1.0 / math.sqrt(HEAD_DIM)
BF16 = jnp.bfloat16
F32 = jnp.float32


def kernel(
    tokens,
    bank_hbm,
    slots,
    w_query,
    w_key,
    w_value,
    w_out,
    out,
    normed,
    bank,
    w_all,
    o_all,
    queries,
    kv,
    attended,
    total,
    stage_sem,
    load_sem,
    w_send,
    w_recv,
    y_send,
    y_recv,
    kv_send_sem,
    kv_recv_sem,
    perm_sem,
):
    seq = lax.axis_index("seq")
    y = lax.axis_index("head")
    half = lax.axis_index("batch")
    p = lax.div(seq, 8)
    z = lax.rem(lax.div(seq, 2), 4)
    c = lax.rem(seq, 2)
    z_next = lax.rem(z + 1, 4)
    z_prev = lax.rem(z + 3, 4)
    z_far = lax.rem(z + 2, 4)

    def device(s, h, b):
        return {"seq": s, "head": h, "batch": b}

    up = device(p * 8 + z_next * 2 + c, y, half)
    down = device(p * 8 + z_prev * 2 + c, y, half)
    flip = (1 - p) * 8 + z * 2 + c
    side = device(flip, y, half)
    other_side = device(flip, y, 1 - half)
    partner = device(p * 8 + z * 2 + 1 - c, y, half)
    cross_up = (1 - p) * 8 + z_next * 2 + c
    cross_down = (1 - p) * 8 + z_prev * 2 + c
    side_up = device(cross_up, y, half)
    side_down = device(cross_down, y, half)
    other_up = device(cross_up, y, 1 - half)
    other_down = device(cross_down, y, 1 - half)
    y_up = device(seq, lax.rem(y + 1, 4), half)
    y_down = device(seq, lax.rem(y + 3, 4), half)
    later = device(lax.rem(seq + 1, 16), y, half)
    earlier = device(lax.rem(seq + 15, 16), y, half)
    quarter = lax.div(seq, 4)
    lane = lax.rem(seq, 4)
    moves = quarter != y
    perm_seq = 4 * y + lane
    perm = device(perm_seq, quarter, half)
    y_next = lax.rem(y + 1, 4)
    y_prev = lax.rem(y + 3, 4)

    def slab(r, q, zz, cc, part=None):
        if r < O_ROUND:
            ref = w_all.at[r, q, zz, cc]
            rows = 128
        else:
            ref = o_all.at[q, zz, cc]
            rows = 512
        if part is None:
            return ref
        return ref.at[pl.ds(part * (rows // 2), rows // 2)]

    def sent(src, dst, ss, rs, to):
        return pltpu.make_async_remote_copy(
            src_ref=src, dst_ref=dst, send_sem=ss, recv_sem=rs, device_id=to, device_id_type=MESH
        )

    def stage(r):
        if r in Q_ROUND:
            parts = [(w_query, Q_ROUND.index(r) * WIDTH, 0, WIDTH)]
        else:
            h = KV_ROUND.index(r)
            parts = [(w_key, h * HEAD_DIM, 0, HEAD_DIM), (w_value, h * HEAD_DIM, HEAD_DIM, HEAD_DIM)]
        return [
            pltpu.make_async_copy(
                w.at[:, pl.ds(start, width)], w_all.at[r, p, z, c, :, pl.ds(at, width)], stage_sem.at[r]
            )
            for w, start, at, width in parts
        ]

    token_copy = pltpu.make_async_copy(tokens, normed, load_sem.at[1])
    bank_copies = [pltpu.make_async_copy(bank_hbm.at[b], bank.at[b], load_sem.at[0]) for b in range(BLOCKS)]
    perm_local = pltpu.make_async_copy(w_out, o_all.at[p, z, c], load_sem.at[2])
    perm_dst = o_all.at[lax.div(perm_seq, 8), lax.rem(lax.div(perm_seq, 2), 4), lax.rem(perm_seq, 2)]
    perm_copy = sent(w_out, perm_dst, perm_sem.at[0], perm_sem.at[1], perm)

    barrier = pltpu.get_barrier_semaphore()
    near = (up, down, side, other_side, partner, side_up, side_down, other_up, other_down)
    for peer in near + (y_up, y_down, later, earlier):
        pl.semaphore_signal(barrier, inc=1, device_id=peer, device_id_type=MESH)

    @pl.when(moves)
    def _():
        pl.semaphore_signal(barrier, inc=1, device_id=perm, device_id_type=MESH)

    for r in range(O_ROUND):
        for copy in stage(r):
            copy.start()
        if r == 1:
            token_copy.start()

    pl.semaphore_wait(barrier, 13 + moves.astype(jnp.int32))

    def w_copy(r, k):
        own = (p, z, c)
        before, after, far = (p, z_prev, c), (p, z_next, c), (p, z_far, c)
        where, part, to = {
            0: (own, None, up),
            1: (own, None, down),
            2: (before, 0, up),
            3: (after, 1, down),
            4: (own, 0, side),
            5: (own, 1, other_side),
            6: (before, 0, side),
            7: (before, 1, other_side),
            8: (after, 0, side),
            9: (after, 1, other_side),
            10: (before, 0, side_up),
            11: (after, 1, other_down),
            12: (own, None, partner),
            13: (before, None, partner),
            14: (after, None, partner),
            15: (far, None, partner),
        }[k]
        ref = slab(r, *where, part)
        return sent(ref, ref, w_send.at[r, SEND_OF[k]], w_recv.at[r, RECV_OF[k]], to)

    def w_region(r, *where):
        return w_all.at[(r, *where)] if r < O_ROUND else o_all.at[where]

    def w_far_side(r):
        ref = w_region(r, 1 - p, slice(None), c)
        return sent(ref, ref, w_send.at[r, SEND_OF[16]], w_recv.at[r, RECV_OF[16]], partner)

    def w_taken(r, group, *where):
        ref = w_region(r, *where)
        sent(ref, ref, w_send.at[r, 0], w_recv.at[r, group], up).wait_recv()

    def w_left(r, group, *where):
        ref = w_region(r, *where)
        sent(ref, ref, w_send.at[r, group], w_recv.at[r, 0], up).wait_send()

    def begin(r):
        if r < O_ROUND:
            pltpu.make_async_copy(w_query.at[:, pl.ds(0, WIDTH)], slab(r, p, z, c), stage_sem.at[r]).wait()
        else:

            @pl.when(moves)
            def _():
                perm_copy.wait_recv()

            @pl.when(jnp.logical_not(moves))
            def _():
                perm_local.wait()

        for k in (0, 1, 4, 5, 12):
            w_copy(r, k).start()

    def relay(r):
        w_taken(r, 0, p, z_prev, c)
        for k in (2, 10, 6, 7, 13):
            w_copy(r, k).start()
        w_taken(r, 1, p, z_next, c)
        for k in (3, 11, 8, 9, 14):
            w_copy(r, k).start()

    def relay_far(r):
        w_taken(r, 2, p, z_far, c)
        w_copy(r, 15).start()

    def cross(r):
        w_taken(r, 3, 1 - p, slice(None), c)
        w_far_side(r).start()

    def arrived(r):
        w_taken(r, 4, slice(None), slice(None), 1 - c)

    def y_copy(n, k):
        h, start, count = PIECES[n]
        whose, part, to = {
            0: (y, None, y_up),
            1: (y, None, y_down),
            2: (y_prev, 0, y_up),
            3: (y_next, 1, y_down),
        }[k]
        rows = pl.ds(start, count) if part is None else pl.ds(start + part * (count // 2), count // 2)
        ref = attended.at[h + 1, whose, rows]
        return sent(ref, ref, y_send.at[n], y_recv.at[n, min(k, 2)], to)

    def y_taken(n, group, whose):
        h, start, count = PIECES[n]
        ref = attended.at[h + 1, whose, pl.ds(start, count)]
        sent(ref, ref, y_send.at[n], y_recv.at[n, group], y_up).wait_recv()

    def share(n):
        for k in (0, 1):
            y_copy(n, k).start()

    def share_relay(n):
        y_taken(n, 0, y_prev)
        y_copy(n, 2).start()
        y_taken(n, 1, y_next)
        y_copy(n, 3).start()

    def share_done(n):
        y_taken(n, 2, lax.rem(y + 2, 4))

    def share_drain(n):
        h, start, count = PIECES[n]
        ref = attended.at[h + 1, pl.ds(0, 3), pl.ds(start, count)]
        sent(ref, ref, y_send.at[n], y_recv.at[n, 0], y_up).wait_send()

    def kv_hand(h):
        return sent(kv.at[KV_OUT + h], kv.at[KV_IN + h + 1], kv_send_sem.at[h], kv_recv_sem.at[h], later)

    def normalize():
        def body(i, carry):
            rows = pl.ds(pl.multiple_of(i * 64, 64), 64)
            hidden = normed[rows, :].astype(F32)
            scale = lax.rsqrt(jnp.mean(hidden * hidden, axis=-1, keepdims=True) + 1e-06)
            normed[rows, :] = (hidden * scale).astype(BF16)
            return carry

        lax.fori_loop(0, ROWS // 64, body, 0)

    def weights(r):
        return w_all[r].reshape(D, WIDTH)

    def project_queries(pair):
        both = jnp.dot(normed[...], weights(1 + 3 * pair), preferred_element_type=F32).astype(BF16)
        queries[2 * pair + 1] = both[:, 0:HEAD_DIM]
        queries[2 * pair + 2] = both[:, HEAD_DIM:WIDTH]

    def place(task):
        return lax.div(task, BLOCKS), lax.rem(task, BLOCKS)

    def scores_of(tasks):
        scores, values = [], []
        for task in tasks:
            slot, position = place(task)
            handed = lax.div(position, BLOCKS - 1)
            rows = kv[handed * (KV_IN + slot) + (1 - handed) * (lax.rem(slot, 2) * BLOCKS + position)]
            block = lax.rem(position + 1, BLOCKS)
            q = queries[slot, pl.ds(pl.multiple_of(block * BLOCK, BLOCK), BLOCK), :]
            scores.append(
                lax.dot_general(q, rows[:, 0:HEAD_DIM], (((1,), (1,)), ((), ())), preferred_element_type=F32) * SCALE
            )
            values.append(rows[:, HEAD_DIM:WIDTH])
        return scores, values

    def probs_of(scores):
        joined = jnp.concatenate(scores, axis=0)
        exponent = jnp.exp(joined - jnp.max(joined, axis=-1, keepdims=True))
        inverse = 1.0 / jnp.sum(exponent, axis=-1, keepdims=True)
        probs = (exponent * inverse).astype(BF16)
        return [probs[n * BLOCK : (n + 1) * BLOCK] for n in range(len(scores))]

    def mix(tasks, probs, values):
        mixed = []
        for task, weight, rows in zip(tasks, probs, values):
            one = jnp.dot(weight, rows, preferred_element_type=F32)
            empty = jnp.logical_and(lax.rem(task, BLOCKS) == BLOCKS - 1, seq == 0)
            mixed.append(jnp.where(empty, jnp.zeros_like(one), one).astype(BF16))
        return mixed

    def keep(tasks, mixed):
        for task, rows in zip(tasks, mixed):
            slot, position = place(task)
            attended[slot, y, pl.ds(pl.multiple_of(position * BLOCK, BLOCK), BLOCK), :] = rows

    def attend(tasks):
        scores, values = scores_of(tasks)
        keep(tasks, mix(tasks, probs_of(scores), values))

    def step(h, i):
        tasks = [BLOCKS * h + STEP * i + BLOCKS - STEP - 1 + n for n in range(STEP)]
        scores, values = scores_of(tasks)
        probs = probs_of(scores)
        blocks = [lax.rem(STEP * i + BLOCKS - 1, BLOCKS)] + [STEP * i + n for n in range(STEP - 1)]
        rows = jnp.concatenate([bank[slots[block]] for block in blocks], axis=0)
        new = jnp.dot(rows, weights(h + lax.div(h + 1, 2)), preferred_element_type=F32).astype(BF16)
        mixed = mix(tasks, probs, values)
        own = lax.rem(h + 1, 2) * BLOCKS
        kept = lax.div(i + STEPS - 1, STEPS)
        kv[(1 - kept) * (KV_OUT + h) + kept * (own + blocks[0])] = new[0:KEYS]
        for n in range(1, STEP):
            kv[own + blocks[n]] = new[n * KEYS : (n + 1) * KEYS]
        keep(tasks, mixed)

    def out_weights(h):
        rows = pl.ds(h * 128, 128)
        return jnp.concatenate(
            [
                jnp.concatenate([o_all[t // 8, (t // 2) % 4, t % 2, rows, :] for t in range(4 * g, 4 * g + 4)], axis=1)
                for g in range(4)
            ],
            axis=0,
        )

    def project_out(n):
        share_done(n)
        h, start, count = PIECES[n]
        rows = pl.ds(start, count)
        wide = jnp.concatenate([attended[h + 1, g, rows, :] for g in range(4)], axis=1)
        added = jnp.dot(wide, out_weights(h), preferred_element_type=F32)
        if h == 0:
            total[rows, :] = added
        elif h < HEADS - 1:
            total[rows, :] += added
        else:
            done = (total[rows, :] + added).astype(BF16)
            if start + count < ROWS:
                out[start + BLOCK : start + BLOCK + count, :] = done
            else:
                out[start + BLOCK : ROWS, :] = done[: count - BLOCK]
                out[0:BLOCK, :] = done[count - BLOCK :]

    def swap_out_weights():
        @pl.when(moves)
        def _():
            perm_copy.start()

        @pl.when(jnp.logical_not(moves))
        def _():
            perm_local.start()

    def load_bank():
        for copy in bank_copies:
            copy.start()

    def catch_up():
        attend([BLOCKS + n for n in range(7)])
        share(0)

    def drain(r):
        w_left(r, 0, slice(None), z, c)
        w_left(r, 1, p, z, c)
        w_left(r, 2, 1 - p, slice(None), c)
        w_left(r, 3, slice(None), slice(None), c)

    begin(0)
    token_copy.wait()
    normalize()
    relay(0)
    begin(1)
    begin(2)
    load_bank()
    relay_far(0)
    relay(1)
    cross(0)
    relay(2)
    begin(3)
    pltpu.make_async_copy(bank_hbm, bank, load_sem.at[0]).wait()
    arrived(0)

    after = {
        0: [(relay_far, 1)],
        1: [(cross, 1), (swap_out_weights,), (begin, 4)],
        2: [(arrived, 1), (project_queries, 0), (catch_up,), (relay_far, 2), (cross, 2), (relay, 3)],
        3: [(share, 1), (arrived, 2), (begin, 5)],
        4: [(relay, 4)],
        5: [(share, 2), (share_relay, 0), (relay_far, 3)],
        6: [(share, 3), (cross, 3), (relay, 5), (share_relay, 1), (begin, 6)],
        7: [(share, 4), (relay_far, 4), (cross, 4), (arrived, 3)],
        8: [(share_relay, 2), (arrived, 4), (project_queries, 1), (relay_far, 5)],
        9: [(share, 5), (cross, 5), (relay, 6)],
        10: [(share, 6), (share_relay, 3)],
        11: [(share, 7), (arrived, 5), (share_relay, 4)],
        12: [(share_relay, 5), (relay_far, 6)],
        13: [(share, 8), (cross, 6)],
        14: [(share, 9), (share_relay, 6)],
        15: [(share, 10)],
    }

    def one_step(n, carry):
        h, i = lax.div(n, STEPS), lax.rem(n, STEPS)
        step(h, i)

        for head in range(HEADS):

            @pl.when(h == head)
            def _(head=head):
                for at in range(STEPS):

                    @pl.when(i == at)
                    def _(at=at):
                        for action, *rest in after[STEPS * head + at]:
                            action(*rest)

        @pl.when(i == 0)
        def _():
            kv_hand(h).start()

            @pl.when(h > 0)
            def _():
                kv_hand(h - 1).wait_recv()

        return carry

    lax.fori_loop(0, STEPS * HEADS, one_step, 0)

    kv_hand(HEADS - 1).wait_recv()
    attend([BLOCKS * HEADS + n for n in (11, 12, 13, 14, 15)])
    arrived(6)
    project_out(0)
    share(11)
    share(12)
    share_relay(7)
    project_out(1)
    project_out(2)
    project_out(3)
    share_relay(8)
    project_out(4)
    project_out(5)
    for r in range(O_ROUND + 1):
        drain(r)
    share_relay(9)
    project_out(6)
    share_relay(10)
    share_relay(11)
    share_relay(12)
    project_out(7)
    project_out(8)
    for n in range(8):
        share_drain(n)
    for h in range(HEADS):
        kv_hand(h).wait_send()
    project_out(9)
    project_out(10)
    project_out(11)
    project_out(12)
    for n in range(8, len(PIECES)):
        share_drain(n)

    @pl.when(moves)
    def _():
        perm_copy.wait_send()


def local(tokens, neighbor_bank, slots, w_query, w_key, w_value, w_out):
    hbm = pl.BlockSpec(memory_space=pltpu.HBM)
    return pl.pallas_call(
        kernel,
        out_shape=jax.ShapeDtypeStruct((ROWS, HEADS * HEAD_DIM), BF16),
        in_specs=[hbm, hbm, pl.BlockSpec(memory_space=pltpu.SMEM), hbm, hbm, hbm, hbm],
        out_specs=pl.BlockSpec(memory_space=pltpu.VMEM),
        scratch_shapes=[
            pltpu.VMEM((ROWS, D), BF16),
            pltpu.VMEM((BLOCKS, KEYS, D), BF16),
            pltpu.VMEM((O_ROUND, 2, 4, 2, 128, WIDTH), BF16),
            pltpu.VMEM((2, 4, 2, 512, 128), BF16),
            pltpu.VMEM((HEADS + 1, ROWS, HEAD_DIM), BF16),
            pltpu.VMEM((KV_OUT + HEADS, KEYS, WIDTH), BF16),
            pltpu.VMEM((HEADS + 1, 4, ROWS, HEAD_DIM), BF16),
            pltpu.VMEM((ROWS, 512), F32),
            pltpu.SemaphoreType.DMA((O_ROUND,)),
            pltpu.SemaphoreType.DMA((3,)),
            pltpu.SemaphoreType.DMA((O_ROUND + 1, 4)),
            pltpu.SemaphoreType.DMA((O_ROUND + 1, 5)),
            pltpu.SemaphoreType.DMA((len(PIECES),)),
            pltpu.SemaphoreType.DMA((len(PIECES), 3)),
            pltpu.SemaphoreType.DMA((HEADS,)),
            pltpu.SemaphoreType.DMA((HEADS,)),
            pltpu.SemaphoreType.DMA((2,)),
        ],
        compiler_params=pltpu.CompilerParams(
            collective_id=0, has_side_effects=True, vmem_limit_bytes=52 * 1024 * 1024
        ),
        name="attention",
    )(*[pltpu.with_memory_space_constraint(a, pltpu.HBM) for a in (tokens, neighbor_bank, slots, w_query, w_key, w_value, w_out)])


def solution(mesh):
    in_specs = (
        P(("batch", "seq"), None),
        P(("batch", "seq"), None, None),
        P(("batch", "seq")),
        P("seq", "head"),
        P("seq", "head"),
        P("seq", "head"),
        P("head", "seq"),
    )
    out_specs = P(("batch", "seq"), "head")
    return jax.shard_map(local, mesh=mesh, in_specs=in_specs, out_specs=out_specs, check_vma=False)
```

```python
import functools
import math

import jax
import jax.numpy as jnp
from jax import lax
from jax.experimental import pallas as pl
from jax.experimental.pallas import tpu as pltpu
from jax.sharding import PartitionSpec as P

MESH = pl.DeviceIdType.MESH
HEAD_DIM = 128
BLOCKS = 16
BLOCK = 64
KEYS = 256
D = 2048
ROWS = BLOCKS * BLOCK
HEADS = 4
PIECES = tuple((h, start * BLOCK, count * BLOCK) for h in range(HEADS) for start, count in ((0, 7), (7, 4), (11, 5)))
PIECES = PIECES[:-1] + ((3, 11 * BLOCK, 3 * BLOCK), (3, 14 * BLOCK, 2 * BLOCK))
WIDTH = 2 * HEAD_DIM
KV_ROUND = (0, 2, 3, 5)
Q_ROUND = (1, 4)
O_ROUND = 6
KV_IN = 2 * BLOCKS
KV_OUT = KV_IN + HEADS + 1
SEND_OF = (0,) * 2 + (1,) * 2 + (2,) * 8 + (3,) * 5
RECV_OF = (0, 1) + (2,) * 2 + (3,) * 8 + (4,) * 5
STEP = 4
STEPS = BLOCKS // STEP
SCALE = 1.0 / math.sqrt(HEAD_DIM)
BF16 = jnp.bfloat16
F32 = jnp.float32


def kernel(
    tokens,
    bank_hbm,
    slots,
    w_query,
    w_key,
    w_value,
    w_out,
    out,
    normed,
    bank,
    w_all,
    o_all,
    queries,
    kv,
    attended,
    total,
    stage_sem,
    load_sem,
    w_send,
    w_recv,
    y_send,
    y_recv,
    kv_send_sem,
    kv_recv_sem,
    perm_sem,
):
    seq = lax.axis_index("seq")
    y = lax.axis_index("head")
    half = lax.axis_index("batch")
    p = lax.div(seq, 8)
    z = lax.rem(lax.div(seq, 2), 4)
    c = lax.rem(seq, 2)
    z_next = lax.rem(z + 1, 4)
    z_prev = lax.rem(z + 3, 4)
    z_far = lax.rem(z + 2, 4)

    def device(s, h, b):
        return {"seq": s, "head": h, "batch": b}

    up = device(p * 8 + z_next * 2 + c, y, half)
    down = device(p * 8 + z_prev * 2 + c, y, half)
    flip = (1 - p) * 8 + z * 2 + c
    side = device(flip, y, half)
    other_side = device(flip, y, 1 - half)
    partner = device(p * 8 + z * 2 + 1 - c, y, half)
    cross_up = (1 - p) * 8 + z_next * 2 + c
    cross_down = (1 - p) * 8 + z_prev * 2 + c
    side_up = device(cross_up, y, half)
    side_down = device(cross_down, y, half)
    other_up = device(cross_up, y, 1 - half)
    other_down = device(cross_down, y, 1 - half)
    y_up = device(seq, lax.rem(y + 1, 4), half)
    y_down = device(seq, lax.rem(y + 3, 4), half)
    later = device(lax.rem(seq + 1, 16), y, half)
    earlier = device(lax.rem(seq + 15, 16), y, half)
    quarter = lax.div(seq, 4)
    lane = lax.rem(seq, 4)
    moves = quarter != y
    perm_seq = 4 * y + lane
    perm = device(perm_seq, quarter, half)
    y_next = lax.rem(y + 1, 4)
    y_prev = lax.rem(y + 3, 4)

    def slab(r, q, zz, cc, part=None):
        if r < O_ROUND:
            ref = w_all.at[r, q, zz, cc]
            rows = 128
        else:
            ref = o_all.at[q, zz, cc]
            rows = 512
        if part is None:
            return ref
        return ref.at[pl.ds(part * (rows // 2), rows // 2)]

    def sent(src, dst, ss, rs, to):
        return pltpu.make_async_remote_copy(
            src_ref=src, dst_ref=dst, send_sem=ss, recv_sem=rs, device_id=to, device_id_type=MESH
        )

    def stage(r):
        if r in Q_ROUND:
            parts = [(w_query, Q_ROUND.index(r) * WIDTH, 0, WIDTH)]
        else:
            h = KV_ROUND.index(r)
            parts = [(w_key, h * HEAD_DIM, 0, HEAD_DIM), (w_value, h * HEAD_DIM, HEAD_DIM, HEAD_DIM)]
        return [
            pltpu.make_async_copy(
                w.at[:, pl.ds(start, width)], w_all.at[r, p, z, c, :, pl.ds(at, width)], stage_sem.at[r]
            )
            for w, start, at, width in parts
        ]

    token_copy = pltpu.make_async_copy(tokens, normed, load_sem.at[1])
    bank_copies = [pltpu.make_async_copy(bank_hbm.at[b], bank.at[b], load_sem.at[0]) for b in range(BLOCKS)]
    perm_local = pltpu.make_async_copy(w_out, o_all.at[p, z, c], load_sem.at[2])
    perm_dst = o_all.at[lax.div(perm_seq, 8), lax.rem(lax.div(perm_seq, 2), 4), lax.rem(perm_seq, 2)]
    perm_copy = sent(w_out, perm_dst, perm_sem.at[0], perm_sem.at[1], perm)

    barrier = pltpu.get_barrier_semaphore()
    near = (up, down, side, other_side, partner, side_up, side_down, other_up, other_down)
    for peer in near + (y_up, y_down, later, earlier):
        pl.semaphore_signal(barrier, inc=1, device_id=peer, device_id_type=MESH)

    @pl.when(moves)
    def _():
        pl.semaphore_signal(barrier, inc=1, device_id=perm, device_id_type=MESH)

    for r in range(O_ROUND):
        for copy in stage(r):
            copy.start()
        if r == 1:
            token_copy.start()

    pl.semaphore_wait(barrier, 13 + moves.astype(jnp.int32))

    def w_copy(r, k):
        own = (p, z, c)
        before, after, far = (p, z_prev, c), (p, z_next, c), (p, z_far, c)
        where, part, to = {
            0: (own, None, up),
            1: (own, None, down),
            2: (before, 0, up),
            3: (after, 1, down),
            4: (own, 0, side),
            5: (own, 1, other_side),
            6: (before, 0, side),
            7: (before, 1, other_side),
            8: (after, 0, side),
            9: (after, 1, other_side),
            10: (before, 0, side_up),
            11: (after, 1, other_down),
            12: (own, None, partner),
            13: (before, None, partner),
            14: (after, None, partner),
            15: (far, None, partner),
        }[k]
        ref = slab(r, *where, part)
        return sent(ref, ref, w_send.at[r // O_ROUND, SEND_OF[k]], w_recv.at[r, RECV_OF[k]], to)

    def w_region(r, *where):
        return w_all.at[(r, *where)] if r < O_ROUND else o_all.at[where]

    def w_far_side(r):
        ref = w_region(r, 1 - p, slice(None), c)
        return sent(ref, ref, w_send.at[r // O_ROUND, SEND_OF[16]], w_recv.at[r, RECV_OF[16]], partner)

    def w_taken(r, group, *where):
        ref = w_region(r, *where)
        sent(ref, ref, w_send.at[0, 0], w_recv.at[r, group], up).wait_recv()

    def w_left(group, *where):
        for last, ref in enumerate((w_all.at[(slice(None), *where)], o_all.at[where])):
            sent(ref, ref, w_send.at[last, group], w_recv.at[0, 0], up).wait_send()

    def begin(r):
        if r < O_ROUND:
            pltpu.make_async_copy(w_query.at[:, pl.ds(0, WIDTH)], slab(r, p, z, c), stage_sem.at[r]).wait()
        else:

            @pl.when(moves)
            def _():
                perm_copy.wait_recv()

            @pl.when(jnp.logical_not(moves))
            def _():
                perm_local.wait()

        for k in (0, 1, 4, 5, 12):
            w_copy(r, k).start()

    def relay(r):
        w_taken(r, 0, p, z_prev, c)
        for k in (2, 10, 6, 7, 13):
            w_copy(r, k).start()
        w_taken(r, 1, p, z_next, c)
        for k in (3, 11, 8, 9, 14):
            w_copy(r, k).start()

    def relay_far(r):
        w_taken(r, 2, p, z_far, c)
        w_copy(r, 15).start()

    def cross(r):
        w_taken(r, 3, 1 - p, slice(None), c)
        w_far_side(r).start()

    def arrived(r):
        w_taken(r, 4, slice(None), slice(None), 1 - c)

    def y_copy(n, k):
        h, start, count = PIECES[n]
        whose, part, to = {
            0: (y, None, y_up),
            1: (y, None, y_down),
            2: (y_prev, 0, y_up),
            3: (y_next, 1, y_down),
        }[k]
        rows = pl.ds(start, count) if part is None else pl.ds(start + part * (count // 2), count // 2)
        ref = attended.at[h + 1, whose, rows]
        return sent(ref, ref, y_send.at[0], y_recv.at[n, min(k, 2)], to)

    def y_taken(n, group, whose):
        h, start, count = PIECES[n]
        ref = attended.at[h + 1, whose, pl.ds(start, count)]
        sent(ref, ref, y_send.at[0], y_recv.at[n, group], y_up).wait_recv()

    def share(n):
        for k in (0, 1):
            y_copy(n, k).start()

    def share_relay(n):
        y_taken(n, 0, y_prev)
        y_copy(n, 2).start()
        y_taken(n, 1, y_next)
        y_copy(n, 3).start()

    def share_done(n):
        y_taken(n, 2, lax.rem(y + 2, 4))

    def share_drain():
        ref = attended.at[pl.ds(1, HEADS), pl.ds(0, 3)]
        sent(ref, ref, y_send.at[0], y_recv.at[0, 0], y_up).wait_send()

    def kv_hand(h):
        return sent(kv.at[KV_OUT + h], kv.at[KV_IN + h + 1], kv_send_sem.at[0], kv_recv_sem.at[h], later)

    def normalize():
        def body(i, carry):
            rows = pl.ds(pl.multiple_of(i * 64, 64), 64)
            hidden = normed[rows, :].astype(F32)
            scale = lax.rsqrt(jnp.mean(hidden * hidden, axis=-1, keepdims=True) + 1e-06)
            normed[rows, :] = (hidden * scale).astype(BF16)
            return carry

        lax.fori_loop(0, ROWS // 64, body, 0)

    def weights(r):
        return w_all[r].reshape(D, WIDTH)

    def project_queries(pair):
        both = jnp.dot(normed[...], weights(1 + 3 * pair), preferred_element_type=F32).astype(BF16)
        queries[2 * pair + 1] = both[:, 0:HEAD_DIM]
        queries[2 * pair + 2] = both[:, HEAD_DIM:WIDTH]

    def place(task):
        return lax.div(task, BLOCKS), lax.rem(task, BLOCKS)

    def scores_of(tasks):
        scores, values = [], []
        for task in tasks:
            slot, position = place(task)
            handed = lax.div(position, BLOCKS - 1)
            rows = kv[handed * (KV_IN + slot) + (1 - handed) * (lax.rem(slot, 2) * BLOCKS + position)]
            block = lax.rem(position + 1, BLOCKS)
            q = queries[slot, pl.ds(pl.multiple_of(block * BLOCK, BLOCK), BLOCK), :]
            scores.append(
                lax.dot_general(q, rows[:, 0:HEAD_DIM], (((1,), (1,)), ((), ())), preferred_element_type=F32) * SCALE
            )
            values.append(rows[:, HEAD_DIM:WIDTH])
        return scores, values

    def probs_of(scores):
        joined = jnp.concatenate(scores, axis=0)
        exponent = jnp.exp(joined - jnp.max(joined, axis=-1, keepdims=True))
        inverse = 1.0 / jnp.sum(exponent, axis=-1, keepdims=True)
        probs = (exponent * inverse).astype(BF16)
        return [probs[n * BLOCK : (n + 1) * BLOCK] for n in range(len(scores))]

    def mix(tasks, probs, values):
        mixed = []
        for task, weight, rows in zip(tasks, probs, values):
            one = jnp.dot(weight, rows, preferred_element_type=F32)
            empty = jnp.logical_and(lax.rem(task, BLOCKS) == BLOCKS - 1, seq == 0)
            mixed.append(jnp.where(empty, jnp.zeros_like(one), one).astype(BF16))
        return mixed

    def keep(tasks, mixed):
        for task, rows in zip(tasks, mixed):
            slot, position = place(task)
            attended[slot, y, pl.ds(pl.multiple_of(position * BLOCK, BLOCK), BLOCK), :] = rows

    def attend(tasks):
        scores, values = scores_of(tasks)
        keep(tasks, mix(tasks, probs_of(scores), values))

    def step(h, i):
        tasks = [BLOCKS * h + STEP * i + BLOCKS - STEP - 1 + n for n in range(STEP)]
        scores, values = scores_of(tasks)
        probs = probs_of(scores)
        blocks = [lax.rem(STEP * i + BLOCKS - 1, BLOCKS)] + [STEP * i + n for n in range(STEP - 1)]
        rows = jnp.concatenate([bank[slots[block]] for block in blocks], axis=0)
        new = jnp.dot(rows, weights(h + lax.div(h + 1, 2)), preferred_element_type=F32).astype(BF16)
        mixed = mix(tasks, probs, values)
        own = lax.rem(h + 1, 2) * BLOCKS
        kept = lax.div(i + STEPS - 1, STEPS)
        kv[(1 - kept) * (KV_OUT + h) + kept * (own + blocks[0])] = new[0:KEYS]
        for n in range(1, STEP):
            kv[own + blocks[n]] = new[n * KEYS : (n + 1) * KEYS]
        keep(tasks, mixed)

    def out_weights(h):
        rows = pl.ds(h * 128, 128)
        return jnp.concatenate(
            [
                jnp.concatenate([o_all[t // 8, (t // 2) % 4, t % 2, rows, :] for t in range(4 * g, 4 * g + 4)], axis=1)
                for g in range(4)
            ],
            axis=0,
        )

    def project_out(n):
        share_done(n)
        h, start, count = PIECES[n]
        rows = pl.ds(start, count)
        wide = jnp.concatenate([attended[h + 1, g, rows, :] for g in range(4)], axis=1)
        added = jnp.dot(wide, out_weights(h), preferred_element_type=F32)
        if h == 0:
            total[rows, :] = added
        elif h < HEADS - 1:
            total[rows, :] += added
        else:
            done = (total[rows, :] + added).astype(BF16)
            if start + count < ROWS:
                out[start + BLOCK : start + BLOCK + count, :] = done
            else:
                out[start + BLOCK : ROWS, :] = done[: count - BLOCK]
                out[0:BLOCK, :] = done[count - BLOCK :]

    def swap_out_weights():
        @pl.when(moves)
        def _():
            perm_copy.start()

        @pl.when(jnp.logical_not(moves))
        def _():
            perm_local.start()

    def load_bank():
        for copy in bank_copies:
            copy.start()

    def catch_up():
        attend([BLOCKS + n for n in range(7)])
        share(0)

    def drain():
        w_left(0, slice(None), z, c)
        w_left(1, p, z, c)
        w_left(2, 1 - p, slice(None), c)
        w_left(3, slice(None), slice(None), c)
        ref = kv.at[pl.ds(KV_OUT, HEADS)]
        sent(ref, ref, kv_send_sem.at[0], kv_recv_sem.at[0], later).wait_send()

    begin(0)
    token_copy.wait()
    normalize()
    relay(0)
    begin(1)
    begin(2)
    load_bank()
    relay_far(0)
    relay(1)
    cross(0)
    relay(2)
    begin(3)
    pltpu.make_async_copy(bank_hbm, bank, load_sem.at[0]).wait()
    arrived(0)

    after = {
        0: [(relay_far, 1)],
        1: [(cross, 1), (swap_out_weights,), (begin, 4)],
        2: [(arrived, 1), (project_queries, 0), (catch_up,), (relay_far, 2), (cross, 2), (relay, 3)],
        3: [(share, 1), (arrived, 2), (begin, 5)],
        4: [(relay, 4)],
        5: [(share, 2), (share_relay, 0), (relay_far, 3)],
        6: [(share, 3), (cross, 3), (relay, 5), (share_relay, 1), (begin, 6)],
        7: [(share, 4), (relay_far, 4), (cross, 4), (arrived, 3)],
        8: [(share_relay, 2), (arrived, 4), (project_queries, 1), (relay_far, 5)],
        9: [(share, 5), (cross, 5), (relay, 6)],
        10: [(share, 6), (share_relay, 3)],
        11: [(share, 7), (arrived, 5), (share_relay, 4)],
        12: [(share_relay, 5), (relay_far, 6)],
        13: [(share, 8), (cross, 6)],
        14: [(share, 9), (share_relay, 6)],
        15: [(share, 10)],
    }

    def one_step(n, carry):
        h, i = lax.div(n, STEPS), lax.rem(n, STEPS)
        step(h, i)

        for head in range(HEADS):

            @pl.when(h == head)
            def _(head=head):
                for at in range(STEPS):

                    @pl.when(i == at)
                    def _(at=at):
                        for action, *rest in after[STEPS * head + at]:
                            action(*rest)

        @pl.when(i == 0)
        def _():
            kv_hand(h).start()

            @pl.when(h > 0)
            def _():
                kv_hand(h - 1).wait_recv()

        return carry

    lax.fori_loop(0, STEPS * HEADS, one_step, 0)

    kv_hand(HEADS - 1).wait_recv()
    attend([BLOCKS * HEADS + n for n in (11, 12, 13, 14, 15)])
    arrived(6)
    project_out(0)
    share(11)
    share(12)
    share_relay(7)
    project_out(1)
    project_out(2)
    project_out(3)
    share_relay(8)
    project_out(4)
    project_out(5)
    drain()
    share_relay(9)
    project_out(6)
    share_relay(10)
    share_relay(11)
    share_relay(12)
    project_out(7)
    project_out(8)
    project_out(9)
    project_out(10)
    project_out(11)
    project_out(12)
    share_drain()

    @pl.when(moves)
    def _():
        perm_copy.wait_send()


def local(tokens, neighbor_bank, slots, w_query, w_key, w_value, w_out):
    hbm = pl.BlockSpec(memory_space=pltpu.HBM)
    return pl.pallas_call(
        kernel,
        out_shape=jax.ShapeDtypeStruct((ROWS, HEADS * HEAD_DIM), BF16),
        in_specs=[hbm, hbm, pl.BlockSpec(memory_space=pltpu.SMEM), hbm, hbm, hbm, hbm],
        out_specs=pl.BlockSpec(memory_space=pltpu.VMEM),
        scratch_shapes=[
            pltpu.VMEM((ROWS, D), BF16),
            pltpu.VMEM((BLOCKS, KEYS, D), BF16),
            pltpu.VMEM((O_ROUND, 2, 4, 2, 128, WIDTH), BF16),
            pltpu.VMEM((2, 4, 2, 512, 128), BF16),
            pltpu.VMEM((HEADS + 1, ROWS, HEAD_DIM), BF16),
            pltpu.VMEM((KV_OUT + HEADS, KEYS, WIDTH), BF16),
            pltpu.VMEM((HEADS + 1, 4, ROWS, HEAD_DIM), BF16),
            pltpu.VMEM((ROWS, 512), F32),
            pltpu.SemaphoreType.DMA((O_ROUND,)),
            pltpu.SemaphoreType.DMA((3,)),
            pltpu.SemaphoreType.DMA((2, 4)),
            pltpu.SemaphoreType.DMA((O_ROUND + 1, 5)),
            pltpu.SemaphoreType.DMA((1,)),
            pltpu.SemaphoreType.DMA((len(PIECES), 3)),
            pltpu.SemaphoreType.DMA((1,)),
            pltpu.SemaphoreType.DMA((HEADS,)),
            pltpu.SemaphoreType.DMA((2,)),
        ],
        compiler_params=pltpu.CompilerParams(
            collective_id=0, has_side_effects=True, vmem_limit_bytes=52 * 1024 * 1024
        ),
        name="attention",
    )(*[pltpu.with_memory_space_constraint(a, pltpu.HBM) for a in (tokens, neighbor_bank, slots, w_query, w_key, w_value, w_out)])


def solution(mesh):
    in_specs = (
        P(("batch", "seq"), None),
        P(("batch", "seq"), None, None),
        P(("batch", "seq")),
        P("seq", "head"),
        P("seq", "head"),
        P("seq", "head"),
        P("head", "seq"),
    )
    out_specs = P(("batch", "seq"), "head")
    return jax.shard_map(local, mesh=mesh, in_specs=in_specs, out_specs=out_specs, check_vma=False)
```
